32 devices in a mesh: ep: 8 (over y, x, core), dp: 4 (over z).
Axes of the slice: x: 2, y: 2, z: 4, core: 2. Of those that a mesh axis runs over, the one named last changes fastest.
Arguments:
- resid: bfloat16 [512, 4096], P(('ep', 'dp')), may hold values from -6 to 6
- queries: bfloat16 [512, 8192], P(('ep', 'dp')), may hold values from -4.5 to 4.5
- new_keys: bfloat16 [512, 512], P(('ep', 'dp')), may hold values from -4.5 to 4.5
- new_values: bfloat16 [512, 512], P(('ep', 'dp')), may hold values from -6 to 6
- cache_keys: bfloat16 [512, 128, 512], P(('ep', 'dp')), may hold values from -4.5 to 4.5
- cache_values: bfloat16 [512, 128, 512], P(('ep', 'dp')), may hold values from -6 to 6
- cache_len: int32 [512], P(('ep', 'dp')), may hold values from 1 to 128
- out_proj: bfloat16 [8192, 4096], P('ep'), may hold values from -0.0625 to 0.0625
- norm_gain: float32 [4096], replicated, may hold values from 0.1 to 1.9
- router: bfloat16 [4096, 16], replicated, may hold values from -4 to 4
- expert_ids: int32 [512, 8], P(('ep', 'dp')), may hold values from 0 to 15, all different within a row; in each aligned block of 16 rows (0 to 15, 16 to 31, ...) at most 14 rows name the same one
- gate_slab: bfloat16 [32, 4096, 384], P(('ep', 'dp')), may hold values from -0.09375 to 0.09375
- up_slab: bfloat16 [32, 4096, 384], P(('ep', 'dp')), may hold values from -0.09375 to 0.09375
- down_slab: bfloat16 [32, 384, 4096], P(('ep', 'dp')), may hold values from -0.21875 to 0.21875
Outputs:
- mixed: float32 [512, 4096], P(('ep', 'dp'))
The draws below stay inside these ranges and needn't reach their ends.
Inputs may be any that keep to these rules, and one draw needn't show every extreme that they name: `expert_ids`: each row names 8 different experts; among the rows of one device no expert is named by more than 14 rows.
All inputs are finite; a program needn't handle non-finite values.
Results may differ from the reference program's by a relative error of at most 0.009.
Values may be sent and summed in bfloat16 or wider, within the bound.
A program may use at most 128 MiB of HBM per device.

```python
import math
import jax
import jax.numpy as jnp
import numpy as np
from jax import lax

D = 4096
H = 64
KVH = 4
HD = 128
TOP = 8
FF = 768
TOK_DEV = 16
CACHE = 128
EXPERTS = 16
HF = 384
CAP = 14
TOKENS = 512
N_EP = 8
DEVICES = 32


edge_value = 4.5


def draw_queries(key, part):
    sampled = jnp.clip(jax.random.normal(jax.random.fold_in(key, 1), (TOKENS, H * HD), jnp.float32), -edge_value, edge_value)
    return sampled.astype(jnp.bfloat16)


def draw_cache_keys(key, part):
    sampled = jnp.clip(jax.random.normal(jax.random.fold_in(key, 2), (TOKENS, CACHE, KVH * HD), jnp.float32), -edge_value, edge_value)
    return sampled.astype(jnp.bfloat16)


def draw_router(key, part):
    sampled = jnp.clip(jax.random.normal(jax.random.fold_in(key, 3), (D, EXPERTS), jnp.float32), -4.0, 4.0) / math.sqrt(D)
    return sampled.astype(jnp.bfloat16)


def with_ends(entries, own_key, low, high):
    place = [jax.random.randint(jax.random.fold_in(own_key, axis), (), 0, length) for axis, length in enumerate(entries.shape)]
    main_axis = entries.shape.index(max(entries.shape))
    neighbour = place[:main_axis] + [(place[main_axis] + 1) % entries.shape[main_axis]] + place[main_axis + 1:]
    return entries.at[tuple(place)].set(low).at[tuple(neighbour)].set(high)


def shard_levels(rng, shape, split, least, high):
    loudness, own = 1.0, jax.random.fold_in(rng, 6)
    for axis_at, parts in split:
        steps = jnp.exp(jax.random.uniform(jax.random.fold_in(own, axis_at), (parts,), jnp.float32, least / len(split), high / len(split)))
        loudness = loudness * jnp.repeat(steps, shape[axis_at] // parts).reshape([-1 if axis == axis_at else 1 for axis in range(len(shape))])
    return loudness


def assign_block(rng, own, number, rows, number_of, top, reach, lean):
    order = jax.random.permutation(rng, number_of)
    heavy_load, ordinary = portions_of(number_of, rows * top, reach, lean, True), portions_of(number_of, rows * top, reach, lean, False)
    places = jnp.arange(number_of)

    def named(sizes, offset_by):
        used = int((sizes > 0).sum())
        fixed = max(1, used // 4)
        passed = fixed + (places - fixed + offset_by * (used - fixed)) % max(1, number_of - fixed)
        return jnp.zeros((number_of,), jnp.int32).at[order[jnp.where(places < fixed, places, passed)]].set(jnp.asarray(sizes, jnp.int32))

    sizes = jnp.where(number % 4 == 0, named(heavy_load, number // 4), named(ordinary, number - number // 4 - 1))
    mixed = jax.random.permutation(jax.random.fold_in(own, 3), number_of)
    donor, sink = mixed[0:number_of // 2 * 2:2], mixed[1:number_of // 2 * 2:2]
    margin = jnp.minimum(sizes[donor] - 1, reach - sizes[sink]) // 2
    margin = jnp.where((donor == order[0]) | (sink == order[0]) | (sizes[sink] == 0), 0, jnp.maximum(margin, 0))
    passed = jax.random.randint(jax.random.fold_in(own, 4), (number_of // 2,), 0, 1 << 20) % (margin + 1)
    sizes = sizes.at[donor].add(-passed).at[sink].add(passed)
    labels = jnp.searchsorted(jnp.cumsum(sizes), jnp.arange(rows * top), side="right").astype(jnp.int32)
    listing = labels.reshape(top, rows).T
    listing = listing[jax.random.permutation(jax.random.fold_in(own, 1), rows)]
    offset_by = jax.random.randint(jax.random.fold_in(own, 2), (rows, 1), 0, top)
    return jnp.take_along_axis(listing, (jnp.arange(top)[None, :] + offset_by) % top, axis=1)


def portions_of(count, total, limit, skew, full):
    portions = [(1 << 20) // math.isqrt(rank ** skew) + 1 for rank in range(1, count + 1)]
    largest = limit if full else min(limit, max(-(-total // count), total * portions[0] // sum(portions)))
    least = 1 if total - largest >= count - 1 else 0
    given, spare = [largest] + [least] * (count - 1), total - largest - least * (count - 1)
    while spare > 0:
        movable = [i for i in range(1, count) if given[i] < largest] or [i for i in range(1, count) if given[i] < limit]
        mass, left = sum([portions[i] for i in movable]), spare
        for i in movable:
            addition = min(limit - given[i], max(1, left * portions[i] // mass), spare)
            given[i] = given[i] + addition
            spare = spare - addition
    return np.array(given)


def scatter_about(key, dims, width, reach, cuts=(), held_as=jnp.bfloat16):
    values = width * jax.random.normal(key, dims, jnp.float32)
    if cuts:
        values = values * shard_levels(key, dims, cuts, -0.22, 0.18)
    return jnp.clip(values, -reach, reach).astype(held_as)


def setup_inputs(seed: int = 0) -> dict:
    seeds = jax.random.split(jax.random.key(seed), 15)
    resid = scatter_about(seeds[0], (TOKENS, D), 1.0, 6.0, ((0, 32),))
    queries = draw_queries(jax.random.fold_in(seeds[14], 71), 0)
    new_keys = scatter_about(seeds[2], (TOKENS, KVH * HD), 1.0, 4.5, ((0, 32),))
    new_values = scatter_about(seeds[3], (TOKENS, KVH * HD), 1.0, 6.0, ((0, 32),))
    cache_keys = draw_cache_keys(jax.random.fold_in(seeds[14], 71), 0)
    cache_values = scatter_about(seeds[5], (TOKENS, CACHE, KVH * HD), 1.0, 6.0, ((0, 32),))
    cache_len = with_ends(jax.random.randint(seeds[6], (TOKENS,), 1, CACHE + 1), jax.random.fold_in(seeds[6], 1), 1, CACHE).astype(jnp.int32)
    out_proj = scatter_about(seeds[7], (H * HD, D), (H * HD) ** -0.5, 0.0625, ((0, 8),))
    norm_gain = jnp.clip(1.0 + 0.18 * jax.random.normal(seeds[8], (D,), jnp.float32), 0.1, 1.9)
    router = draw_router(jax.random.fold_in(seeds[14], 71), 0)
    expert_ids_keys = jax.random.split(jax.random.fold_in(seeds[10], 1), TOKENS // TOK_DEV)
    expert_ids_turns = jax.random.permutation(jax.random.fold_in(seeds[10], 3), TOKENS // TOK_DEV)
    expert_ids = jax.vmap(lambda own, number: assign_block(jax.random.fold_in(seeds[10], 2), own, number, TOK_DEV, EXPERTS, TOP, CAP, 2))(expert_ids_keys, expert_ids_turns).reshape((TOKENS, TOP))
    gate_slab = scatter_about(seeds[11], (DEVICES, D, HF), D ** -0.5, 0.09375, ((0, 32),))
    up_slab = scatter_about(seeds[12], (DEVICES, D, HF), D ** -0.5, 0.09375, ((0, 32),))
    down_slab = scatter_about(seeds[13], (DEVICES, HF, D), FF ** -0.5, 0.21875, ((0, 32),))
    return {"resid": resid, "queries": queries, "new_keys": new_keys, "new_values": new_values, "cache_keys": cache_keys, "cache_values": cache_values, "cache_len": cache_len, "out_proj": out_proj, "norm_gain": norm_gain, "router": router, "expert_ids": expert_ids, "gate_slab": gate_slab, "up_slab": up_slab, "down_slab": down_slab}


def attend_block(query_rows, key_new, value_new, key_cache, value_cache, lengths):
    local_rows = query_rows.shape[0]
    cache_span = key_cache.shape[1]
    group_size = H // KVH
    query_heads = query_rows.astype(jnp.float32).reshape(local_rows, KVH, group_size, HD)
    past_keys = key_cache.astype(jnp.float32).reshape(local_rows, cache_span, KVH, HD)
    past_values = value_cache.astype(jnp.float32).reshape(local_rows, cache_span, KVH, HD)
    score_scale = 1.0 / math.sqrt(HD)
    past_scores = jnp.einsum('tgqd,tcgd->tgqc', query_heads, past_keys) * score_scale
    own_scores = jnp.einsum('tgqd,tgd->tgq', query_heads, key_new.astype(jnp.float32).reshape(local_rows, KVH, HD)) * score_scale
    is_valid = lax.broadcasted_iota(jnp.int32, (local_rows, cache_span), 1) < lengths[:, None]
    past_scores = jnp.where(is_valid[:, None, None, :], past_scores, -1e+30)
    peak_score = jnp.maximum(lax.optimization_barrier(jnp.max(past_scores, axis=3)), own_scores)
    past_exp = jnp.exp(past_scores - peak_score[..., None])
    own_exp = jnp.exp(own_scores - peak_score)
    denom_sum = lax.optimization_barrier(jnp.sum(past_exp, axis=3)) + own_exp
    past_weights = lax.optimization_barrier((past_exp / denom_sum[..., None]).astype(jnp.bfloat16))
    own_weights = lax.optimization_barrier((own_exp / denom_sum).astype(jnp.bfloat16))
    blended = jnp.einsum('tgqc,tcgd->tgqd', past_weights.astype(jnp.float32), past_values)
    blended = blended + own_weights.astype(jnp.float32)[..., None] * value_new.astype(jnp.float32).reshape(local_rows, KVH, 1, HD)
    return blended.reshape(local_rows, H * HD).astype(jnp.bfloat16)

def attend_packed(packed):
    return attend_block(*packed)

def blocked(array):
    return array.reshape((DEVICES, TOK_DEV) + array.shape[1:])

def reference(resid, queries, new_keys, new_values, cache_keys, cache_values, cache_len, out_proj, norm_gain, router, expert_ids, gate_slab, up_slab, down_slab):
    packed = (blocked(queries), blocked(new_keys), blocked(new_values), blocked(cache_keys), blocked(cache_values), blocked(cache_len))
    attended = lax.map(attend_packed, packed).reshape(TOKENS, H * HD)
    column_width = H * HD // N_EP
    attn_out = jnp.zeros((TOKENS, D), jnp.float32)
    for shard_index in range(N_EP):
        row_start = shard_index * column_width
        product = jnp.dot(attended[:, row_start:row_start + column_width], out_proj[row_start:row_start + column_width], preferred_element_type=jnp.float32)
        rounded = lax.optimization_barrier(product.astype(jnp.bfloat16))
        attn_out = attn_out + rounded.astype(jnp.float32)
    hidden = resid.astype(jnp.float32) + attn_out
    meansq = lax.optimization_barrier(jnp.mean(hidden * hidden, axis=1, keepdims=True))
    normed = (hidden * lax.rsqrt(jnp.maximum(meansq, 0.25)) * norm_gain).astype(jnp.bfloat16)
    logits = jnp.dot(normed, router, preferred_element_type=jnp.float32)
    chosen = jnp.take_along_axis(logits, expert_ids.astype(jnp.int32), axis=1)
    peak_logit = lax.optimization_barrier(jnp.max(chosen, axis=1, keepdims=True))
    exp_logit = jnp.exp(chosen - peak_logit)
    gate_probs = lax.optimization_barrier((exp_logit / lax.optimization_barrier(jnp.sum(exp_logit, axis=1, keepdims=True))).astype(jnp.bfloat16))
    flat_ids = expert_ids.reshape(-1).astype(jnp.int32)
    token_of = (jnp.arange(TOKENS * TOP, dtype=jnp.int32) // TOP).astype(jnp.int32)
    onehot = (flat_ids[:, None] == jnp.arange(EXPERTS, dtype=jnp.int32)[None, :]).astype(jnp.int32)
    earlier = jnp.cumsum(onehot, axis=0).astype(jnp.int32) - onehot
    ranking = lax.optimization_barrier(jnp.sum(earlier * onehot, axis=1)).astype(jnp.int32)
    row_depth = DEVICES * CAP
    row_table = jnp.zeros((EXPERTS, row_depth), jnp.int32).at[flat_ids, ranking].set(token_of)

    def run_expert(expert):
        rows_in = jnp.take(normed, row_table[expert], axis=0)
        gate_full = jnp.concatenate((gate_slab[2 * expert], gate_slab[2 * expert + 1]), axis=1)
        up_full = jnp.concatenate((up_slab[2 * expert], up_slab[2 * expert + 1]), axis=1)
        down_full = jnp.concatenate((down_slab[2 * expert], down_slab[2 * expert + 1]), axis=0)
        gate_val = jnp.dot(rows_in, gate_full, preferred_element_type=jnp.float32)
        up_val = jnp.dot(rows_in, up_full, preferred_element_type=jnp.float32)
        activated = (jax.nn.silu(gate_val) * up_val).astype(jnp.bfloat16)
        return jnp.dot(activated, down_full, preferred_element_type=jnp.float32).astype(jnp.bfloat16)
    produced = lax.map(run_expert, jnp.arange(EXPERTS, dtype=jnp.int32))
    picked = produced[flat_ids, ranking].reshape(TOKENS, TOP, D)
    expert_mix = jnp.einsum('tk,tkd->td', gate_probs.astype(jnp.float32), picked.astype(jnp.float32))
    return hidden + expert_mix
```

```python
import math

import jax
import jax.numpy as jnp
from jax import lax
from jax.experimental import pallas as pl
from jax.experimental.pallas import tpu as pltpu
from jax.sharding import PartitionSpec as P

D = 4096
H = 64
KVH = 4
HD = 128
TOP = 8


def attend(queries, new_keys, new_values, cache_keys, cache_values, cache_len):
    local_rows = queries.shape[0]
    cache_span = cache_keys.shape[1]
    group_size = H // KVH
    query_heads = queries.reshape(local_rows, KVH, group_size, HD)
    past_keys = cache_keys.reshape(local_rows, cache_span, KVH, HD)
    past_values = cache_values.reshape(local_rows, cache_span, KVH, HD)
    score_scale = 1.0 / math.sqrt(HD)
    past_scores = (
        jnp.einsum("tgqd,tcgd->tgqc", query_heads, past_keys, preferred_element_type=jnp.float32)
        * score_scale
    )
    own_scores = (
        jnp.einsum(
            "tgqd,tgd->tgq",
            query_heads,
            new_keys.reshape(local_rows, KVH, HD),
            preferred_element_type=jnp.float32,
        )
        * score_scale
    )
    is_valid = lax.broadcasted_iota(jnp.int32, (local_rows, cache_span), 1) < cache_len[:, None]
    past_scores = jnp.where(is_valid[:, None, None, :], past_scores, -1e30)
    peak_score = jnp.maximum(jnp.max(past_scores, axis=3), own_scores)
    past_exp = jnp.exp(past_scores - peak_score[..., None])
    own_exp = jnp.exp(own_scores - peak_score)
    denom_sum = jnp.sum(past_exp, axis=3) + own_exp
    past_weights = (past_exp / denom_sum[..., None]).astype(jnp.bfloat16)
    own_weights = (own_exp / denom_sum).astype(jnp.bfloat16)
    blended = jnp.einsum(
        "tgqc,tcgd->tgqd", past_weights, past_values, preferred_element_type=jnp.float32
    )
    blended = blended + own_weights.astype(jnp.float32)[..., None] * new_values.reshape(
        local_rows, KVH, 1, HD
    ).astype(jnp.float32)
    return blended.reshape(local_rows, H * HD).astype(jnp.bfloat16)


MESH = pl.DeviceIdType.MESH
VMEM_LIMIT = 66_000_000


class Place:
    def __init__(self, side, depth):
        self.side, self.depth = side, depth
        ep = lax.axis_index("ep")
        self.ep = ep
        self.core = lax.rem(ep, 2)
        self.x = lax.rem(ep // 2, side)
        self.y = ep // (2 * side)
        self.z = lax.axis_index("dp")

    def at(self, dy=0, dx=0, dz=0, flip=False):
        y, x = self.line(dy, dx)
        z = lax.rem(self.z + dz, self.depth) if dz else self.z
        core = 1 - self.core if flip else self.core
        return ((y * self.side + x) * 2 + core, z)

    def line(self, dy, dx):
        return lax.rem(self.y + dy, self.side), lax.rem(self.x + dx, self.side)


def greet(devices):
    barrier = pltpu.get_barrier_semaphore()
    for device in devices:
        pl.semaphore_signal(barrier, inc=1, device_id=device, device_id_type=MESH)
    pl.semaphore_wait(barrier, len(devices))


def remote(src, dst, send, recv, device):
    return pltpu.make_async_remote_copy(
        src_ref=src, dst_ref=dst, send_sem=send, recv_sem=recv, device_id=device, device_id_type=MESH
    )


def slices_of(width, extra=0):
    step = 512
    cuts = [[start, step] for start in range(0, width, step)]
    cuts[-1][1] += extra
    return cuts


def reduce_shapes(side, depth, rows, width):
    n = width // 512
    lines = side * side
    bf, dma = jnp.bfloat16, pltpu.SemaphoreType.DMA
    tall = depth * rows
    return [
        pltpu.VMEM((side, side, tall, width), bf),
        pltpu.VMEM((side - 1, side, tall, width), bf),
        pltpu.VMEM((side - 1, tall, width), bf),
        pltpu.VMEM((max(depth - 1, 1), rows, width), bf),
        dma((n, 2)),
        dma((n, side, side, 2)),
        dma((n, side, 2)),
        dma((n, depth, 2)),
    ]


def reduce_phases(here, rows, width, produce, finish, part, scratch, sends):
    in1, in2, in3, in4, sem1, sem2, sem3, sem4 = scratch
    side, depth = here.side, here.depth
    cuts = slices_of(width)

    def rows_of(z):
        return pl.ds(pl.multiple_of(z * rows, rows), rows)

    def core_copy(s):
        start, size = cuts[s]
        cols = pl.ds(start, size)
        return remote(
            part.at[:, :, 1 - here.core, :, cols],
            in1.at[:, :, :, cols],
            sem1.at[s, 0],
            sem1.at[s, 1],
            here.at(flip=True),
        )

    def offsets(s, a, b):
        return (a, b) if s % 2 == 0 else (b, a)

    def first_copy(s, ja, kb, sending):
        cols = pl.ds(*cuts[s])
        slot = side - ja - 1
        y, x = here.line(*offsets(s, ja, kb))
        return remote(
            in1.at[y, x, :, cols],
            in2.at[slot, kb, :, cols],
            sem2.at[s, ja, kb, 0],
            sem2.at[s, side - ja if sending else ja, kb, 1],
            here.at(*offsets(s, ja, 0)),
        )

    def second_copy(s, kb, sending):
        cols = pl.ds(*cuts[s])
        y, x = here.line(*offsets(s, 0, kb))
        return remote(
            in1.at[y, x, :, cols],
            in3.at[side - kb - 1, :, cols],
            sem3.at[s, kb, 0],
            sem3.at[s, side - kb if sending else kb, 1],
            here.at(*offsets(s, 0, kb)),
        )

    def depth_copy(s, jz, sending):
        cols = pl.ds(*cuts[s])
        return remote(
            in1.at[here.y, here.x, rows_of(lax.rem(here.z + jz, depth)), cols],
            in4.at[depth - jz - 1, :, cols],
            sem4.at[s, jz, 0],
            sem4.at[s, depth - jz if sending else jz, 1],
            here.at(0, 0, jz),
        )

    def go(copy):
        copy.start()
        sends.append(copy)

    def wide(value):
        return value.astype(jnp.float32)

    def phase0(s):
        cols = pl.ds(*cuts[s])
        value = produce(s, cols)
        part[:, :, :, :, cols] = value.astype(jnp.bfloat16).reshape(
            side, side, 2, depth * rows, cuts[s][1]
        )
        go(core_copy(s))

    def phase1(s):
        cols = pl.ds(*cuts[s])
        core_copy(s).wait_recv()
        for a in list(range(1, side)) + [0]:
            for b in list(range(1, side)) + [0]:
                y, x = here.line(*offsets(s, a, b))
                total = wide(part[y, x, here.core, :, cols]) + wide(in1[y, x, :, cols])
                in1[y, x, :, cols] = total.astype(jnp.bfloat16)
                if a:
                    go(first_copy(s, a, b, True))

    def phase2(s):
        cols = pl.ds(*cuts[s])
        for b in list(range(1, side)) + [0]:
            y, x = here.line(*offsets(s, 0, b))
            total = wide(in1[y, x, :, cols])
            for a in range(1, side):
                first_copy(s, a, b, False).wait_recv()
                total = total + wide(in2[a - 1, b, :, cols])
            in1[y, x, :, cols] = total.astype(jnp.bfloat16)
            if b:
                go(second_copy(s, b, True))

    def phase3(s):
        cols = pl.ds(*cuts[s])
        total = wide(in1[here.y, here.x, :, cols])
        for b in range(1, side):
            second_copy(s, b, False).wait_recv()
            total = total + wide(in3[b - 1, :, cols])
        if depth == 1:
            finish(s, cols, total)
            return
        in1[here.y, here.x, :, cols] = total.astype(jnp.bfloat16)
        for jz in range(1, depth):
            go(depth_copy(s, jz, True))

    def phase4(s):
        cols = pl.ds(*cuts[s])
        total = wide(in1[here.y, here.x, rows_of(here.z), cols])
        for jz in range(1, depth):
            depth_copy(s, jz, False).wait_recv()
            total = total + wide(in4[jz - 1, :, cols])
        finish(s, cols, total)

    if depth == 1:
        return phase0, phase1, phase2, phase3
    return phase0, phase1, phase2, phase3, phase4


def gather_phases(here, held, rows, width, extra, consume, zsem, lsem, csem, send_sem, sends):
    side, depth = here.side, here.depth
    cuts = slices_of(width, extra)

    def rows_of(z):
        return pl.ds(pl.multiple_of(z * rows, rows), rows)

    def go(copy):
        copy.start()
        sends.append(copy)

    def depth_copy(s, j, sending):
        z = here.z if sending else lax.rem(here.z + j, depth)
        ref = held.at[here.y, here.x, here.core, rows_of(z), pl.ds(*cuts[s])]
        return remote(
            ref, ref, zsem.at[s, j, 0], zsem.at[s, depth - j if sending else j, 1], here.at(0, 0, j)
        )

    def line_ref(s, ky, kx, core):
        y, x = here.line(ky, kx)
        return held.at[y, x, core, :, pl.ds(*cuts[s])]

    def plane_send(s, ky, kx, jy, jx):
        ref = line_ref(s, ky, kx, here.core)
        go(
            remote(
                ref,
                ref,
                send_sem.at[s, ky, kx, jy, jx],
                lsem.at[s, (ky - jy) % side, (kx - jx) % side],
                here.at(jy, jx),
            )
        )

    def core_send(s, ky, kx):
        ref = line_ref(s, ky, kx, here.core)
        go(remote(ref, ref, csem.at[s, ky, kx, 0], csem.at[s, ky, kx, 1], here.at(flip=True)))

    def plane_wait(s, ky, kx):
        ref = line_ref(s, ky, kx, here.core)
        remote(ref, ref, send_sem.at[s, 0, 0, 0, 0], lsem.at[s, ky, kx], here.at(flip=True)).wait_recv()

    def core_wait(s, ky, kx):
        ref = line_ref(s, ky, kx, 1 - here.core)
        remote(ref, ref, csem.at[s, ky, kx, 0], csem.at[s, ky, kx, 1], here.at(flip=True)).wait_recv()

    def turn(s, a, b):
        return (a, b) if s % 2 == 0 else (b, a)

    def phase1(s):
        for j in range(1, depth):
            depth_copy(s, j, False).wait_recv()
        for j in range(1, side):
            plane_send(s, 0, 0, *turn(s, j, 0))
            plane_send(s, 0, 0, *turn(s, 0, j))
        core_send(s, 0, 0)

    def phase2(s):
        for k in range(1, side):
            plane_wait(s, *turn(s, k, 0))
            for j in range(1, side):
                plane_send(s, *turn(s, k, 0), *turn(s, 0, j))
            core_send(s, *turn(s, k, 0))

    def phase3(s):
        for b in range(1, side):
            for a in range(side):
                plane_wait(s, *turn(s, a, b))
                core_send(s, *turn(s, a, b))

    def phase0(s):
        for j in range(1, depth):
            go(depth_copy(s, j, True))

    def phase4(s):
        for a in range(side):
            for b in range(side):
                core_wait(s, a, b)
        consume(s)

    return phase0, phase1, phase2, phase3, phase4


def run_in_order(groups):
    tasks = []
    for phases, count, starts, paces in groups:
        last = [-1.0] * count
        for phase, start, pace in zip(phases, starts, paces):
            for s in range(count):
                last[s] = max(last[s] + 1e-6, start + pace * s)
                tasks.append((last[s], len(tasks), phase, s))
    for _, _, phase, s in sorted(tasks, key=lambda task: task[:2]):
        phase(s)


def layer_kernel(
    side, depth, attended, resid, gain, router, named_ids, proj_hbm, gate_hbm, up_hbm, down_hbm, mixed,
    proj, gate, up, down, regrouped, part, hidden, held, act, gate_sum, up_sum,
    wsem, ssem, rsem, zsem, lsem, csem, send_sem, *scratch
):
    here, flat = Place(side, depth), Place(side, 1)
    rows, features = resid.shape
    experts = router.shape[0]
    count = 2 * side * side
    width = attended.shape[1] // count
    loads = [
        pltpu.make_async_copy(src, dst, wsem.at[i])
        for i, (src, dst) in enumerate(
            ((proj_hbm, proj), (gate_hbm.at[0], gate), (up_hbm.at[0], up), (down_hbm.at[0], down))
        )
    ]
    for load in loads:
        load.start()

    def peer(j):
        return lax.rem(here.ep + j, count)

    greet([(peer(j), here.z) for j in range(1, count)] + [here.at(0, 0, j) for j in range(1, depth)])

    def piece(index):
        return attended.at[:, pl.ds(pl.multiple_of(index * width, 128), width)]

    def exchange(j, sending):
        return remote(
            piece(peer(j)),
            regrouped.at[here.ep] if sending else regrouped.at[peer(j)],
            ssem.at[j],
            rsem.at[count - j if sending else j],
            (peer(j), here.z),
        )

    sends = [exchange(j, True) for j in range(1, count)]
    for copy in sends:
        copy.start()
    regrouped[here.ep] = attended[:, pl.ds(pl.multiple_of(here.ep * width, 128), width)]

    eye = jnp.where(
        lax.broadcasted_iota(jnp.int32, (rows, rows), 0) == lax.broadcasted_iota(jnp.int32, (rows, rows), 1), 1.0, 0.0
    ).astype(jnp.bfloat16)
    label = lax.broadcasted_iota(jnp.int32, (experts, rows), 0)
    hits = jnp.zeros((experts, rows), jnp.float32)
    for k in range(TOP):
        hits = hits + jnp.where(label == named_ids[k : k + 1, :], 1.0, 0.0)
    named = nt_dot(eye, hits.astype(jnp.bfloat16)) > 0.5

    loads[0].wait()
    for j in range(1, count):
        exchange(j, False).wait_recv()

    def produce_proj(s, cols):
        left = regrouped[...].reshape(count * rows, width)
        return jnp.dot(left, proj[:, cols], preferred_element_type=jnp.float32)

    squares, logits = [], []
    slices = len(slices_of(features))
    tail_width = held.shape[-1] - features
    mine = pl.ds(pl.multiple_of(here.z * rows, rows), rows)

    def finish_proj(s, cols, total):
        value = resid[:, cols].astype(jnp.float32) + total
        hidden[:, cols] = value
        scaled = (value * gain[:, cols]).astype(jnp.bfloat16)
        held[here.y, here.x, here.core, mine, cols] = scaled
        if s < slices - 1:
            gather[0](s)
        squares.append(jnp.sum(value * value, axis=1, keepdims=True))
        logits.append(nt_dot(scaled, router[:, cols]))
        if s == slices - 1:
            scale = lax.rsqrt(jnp.maximum(sum(squares) / features, 0.25))
            scores = sum(logits) * scale
            peak = jnp.max(jnp.where(named, scores, -jnp.inf), axis=1, keepdims=True)
            grown = jnp.where(named, jnp.exp(jnp.where(named, scores - peak, 0.0)), 0.0)
            probs = grown / jnp.sum(grown, axis=1, keepdims=True)
            high = scale.astype(jnp.bfloat16).astype(jnp.float32)
            lane = lax.broadcasted_iota(jnp.int32, (rows, tail_width), 1)
            tail = jnp.where(lane == experts, high, jnp.where(lane == experts + 1, scale - high, 0.0))
            held[here.y, here.x, here.core, mine, features:] = tail.astype(jnp.bfloat16)
            held[here.y, here.x, here.core, mine, features : features + experts] = probs.astype(jnp.bfloat16)
            gather[0](s)

    group = side * 2 * depth * rows

    def rows_at(y):
        return pl.ds(pl.multiple_of(y * group, group), group)

    def consume(s):
        if s == 0:
            loads[1].wait()
            loads[2].wait()
        start = 512 * s

        def step(y, carry):
            block = held[y, :, :, :, start : start + 512].reshape(group, 512)
            for weight, total in ((gate, gate_sum), (up, up_sum)):
                value = jnp.dot(
                    block, weight[start : start + 512, :], preferred_element_type=jnp.float32
                )
                total[rows_at(y), :] = value if s == 0 else total[rows_at(y), :] + value
            return carry

        lax.fori_loop(0, side, step, 0)

    proj_scratch, expert_scratch = scratch[: len(scratch) // 2], scratch[len(scratch) // 2 :]
    reduce = reduce_phases(flat, rows, features, produce_proj, finish_proj, part, proj_scratch, sends)
    gather = gather_phases(
        here, held, rows, features, tail_width, consume, zsem, lsem, csem, send_sem, sends
    )
    run_in_order(
        (
            (reduce, slices, PROJ_START, PROJ_PACE),
            (gather[1:], slices, GATHER_START, GATHER_PACE),
        )
    )
    loads[3].wait()
    for copy in sends:
        copy.wait_send()
    sends.clear()
    expert = (here.ep * depth + here.z) // 2

    def activate(y, carry):
        tail = held[y, :, :, :, features:].reshape(group, tail_width).astype(jnp.float32)
        lane = lax.broadcasted_iota(jnp.int32, tail.shape, 1)
        weight = jnp.sum(jnp.where(lane == expert, tail, 0.0), axis=1, keepdims=True)
        scale = jnp.sum(
            jnp.where((lane == experts) | (lane == experts + 1), tail, 0.0), axis=1, keepdims=True
        )
        gate_val = gate_sum[rows_at(y), :] * scale
        value = gate_val / (1.0 + jnp.exp(-gate_val)) * (up_sum[rows_at(y), :] * (scale * weight))
        act[rows_at(y), :] = value.astype(jnp.bfloat16)
        return carry

    lax.fori_loop(0, side, activate, 0)

    def produce(s, cols):
        return jnp.dot(act[...], down[:, cols], preferred_element_type=jnp.float32)

    def finish(s, cols, total):
        mixed[:, cols] = hidden[:, cols] + total

    spread = reduce_phases(here, rows, features, produce, finish, held, expert_scratch, sends)
    run_in_order(((spread, slices, SPREAD_START, SPREAD_PACE),))
    for copy in sends:
        copy.wait_send()


PROJ_START, PROJ_PACE = (0.0, 1.5, 4.5, 7.5), (0.3, 0.5, 0.5, 0.5)
GATHER_START, GATHER_PACE = (11.5, 14.5, 16.5, 18.0), (1.2, 1.75, 1.75, 1.75)
SPREAD_START, SPREAD_PACE = (0.0, 1.5, 5.0, 8.0, 12.0), (0.5, 1.75, 1.75, 1.75, 1.75)


def nt_dot(left, right):
    return lax.dot_general(left, right, (((1,), (1,)), ((), ())), preferred_element_type=jnp.float32)


def run_layer(side, depth, attended, resid, gain, router, named_ids, out_proj, gate_slab, up_slab, down_slab):
    rows, width = resid.shape
    n = width // 512
    experts = router.shape[0]
    bf, dma = jnp.bfloat16, pltpu.SemaphoreType.DMA
    plane = 2 * side * side
    count = plane * depth
    tail = pl.cdiv(experts + 2, 128) * 128
    vmem, anywhere = pl.BlockSpec(memory_space=pltpu.VMEM), pl.BlockSpec(memory_space=pl.ANY)
    return pl.pallas_call(
        lambda *refs: layer_kernel(side, depth, *refs),
        out_shape=jax.ShapeDtypeStruct((rows, width), jnp.float32),
        in_specs=[vmem] * 5 + [anywhere] * 4,
        out_specs=vmem,
        scratch_shapes=[
            pltpu.VMEM(out_proj.shape, bf),
            pltpu.VMEM(gate_slab.shape[1:], bf),
            pltpu.VMEM(up_slab.shape[1:], bf),
            pltpu.VMEM(down_slab.shape[1:], bf),
            pltpu.VMEM((plane, rows, attended.shape[1] // plane), bf),
            pltpu.VMEM((side, side, 2, rows, width), bf),
            pltpu.VMEM((rows, width), jnp.float32),
            pltpu.VMEM((side, side, 2, depth * rows, width + tail), bf),
            pltpu.VMEM((count * rows, gate_slab.shape[2]), bf),
            pltpu.VMEM((count * rows, gate_slab.shape[2]), jnp.float32),
            pltpu.VMEM((count * rows, gate_slab.shape[2]), jnp.float32),
            dma((4,)),
            dma((plane,)),
            dma((plane,)),
            dma((n, depth, 2)),
            dma((n, side, side)),
            dma((n, side, side, 2)),
            dma((n, side, side, side, side)),
        ]
        + reduce_shapes(side, 1, rows, width)
        + reduce_shapes(side, depth, rows, width),
        compiler_params=pltpu.CompilerParams(
            collective_id=0, has_side_effects=True, vmem_limit_bytes=VMEM_LIMIT
        ),
    )(attended, resid, gain, router, named_ids, out_proj, gate_slab, up_slab, down_slab)


def local(
    resid,
    queries,
    new_keys,
    new_values,
    cache_keys,
    cache_values,
    cache_len,
    out_proj,
    norm_gain,
    router,
    expert_ids,
    gate_slab,
    up_slab,
    down_slab,
):
    attended = attend(queries, new_keys, new_values, cache_keys, cache_values, cache_len)
    side = math.isqrt(lax.axis_size("ep") // 2)
    depth = lax.axis_size("dp")
    return run_layer(
        side, depth, attended, resid, norm_gain.reshape(1, -1), router.T, expert_ids.T,
        out_proj, gate_slab, up_slab, down_slab,
    )


def solution(mesh):
    in_specs = (
        P(("ep", "dp"), None),
        P(("ep", "dp"), None),
        P(("ep", "dp"), None),
        P(("ep", "dp"), None),
        P(("ep", "dp"), None, None),
        P(("ep", "dp"), None, None),
        P(("ep", "dp")),
        P("ep", None),
        P(),
        P(),
        P(("ep", "dp"), None),
        P(("ep", "dp"), None, None),
        P(("ep", "dp"), None, None),
        P(("ep", "dp"), None, None),
    )
    out_specs = P(("ep", "dp"), None)
    return jax.shard_map(local, mesh=mesh, in_specs=in_specs, out_specs=out_specs, check_vma=False)
```

```python
import math

import jax
import jax.numpy as jnp
from jax import lax
from jax.experimental import pallas as pl
from jax.experimental.pallas import tpu as pltpu
from jax.sharding import PartitionSpec as P

D = 4096
H = 64
KVH = 4
HD = 128
TOP = 8


MESH = pl.DeviceIdType.MESH
VMEM_LIMIT = 67_000_000


class Place:
    def __init__(self, side, depth):
        self.side, self.depth = side, depth
        ep = lax.axis_index("ep")
        self.ep = ep
        self.core = lax.rem(ep, 2)
        self.x = lax.rem(ep // 2, side)
        self.y = ep // (2 * side)
        self.z = lax.axis_index("dp")

    def at(self, dy=0, dx=0, dz=0, flip=False):
        y, x = self.line(dy, dx)
        z = lax.rem(self.z + dz, self.depth) if dz else self.z
        core = 1 - self.core if flip else self.core
        return ((y * self.side + x) * 2 + core, z)

    def line(self, dy, dx):
        return lax.rem(self.y + dy, self.side), lax.rem(self.x + dx, self.side)


def announce(devices):
    barrier = pltpu.get_barrier_semaphore()
    for device in devices:
        pl.semaphore_signal(barrier, inc=1, device_id=device, device_id_type=MESH)


def gathered(devices):
    pl.semaphore_wait(pltpu.get_barrier_semaphore(), len(devices))


def remote(src, dst, send, recv, device):
    return pltpu.make_async_remote_copy(
        src_ref=src, dst_ref=dst, send_sem=send, recv_sem=recv, device_id=device, device_id_type=MESH
    )


def slices_of(width):
    sizes = [512] * (width // 512)
    sizes = [256, 256] + sizes[2:] + [256, 256]
    cuts, start = [], 0
    for size in sizes:
        cuts.append((start, size))
        start += size
    return cuts


def reduce_shapes(side, depth, rows, width):
    bf, tall = jnp.bfloat16, depth * rows
    return [
        pltpu.VMEM((side, side, tall, width), bf),
        pltpu.VMEM((side - 1, side, tall, width), bf),
        pltpu.VMEM((side - 1, tall, width), bf),
        pltpu.VMEM((max(depth - 1, 1), rows, width), bf),
    ]


def reduce_sems(side, n):
    dma = pltpu.SemaphoreType.DMA
    return [dma((4,)), dma((n,)), dma((n, side - 1, side)), dma((n, side - 1)), dma((n,))]


def wide(value):
    return value.astype(jnp.float32)


def wait_bytes(ref, sem):
    pltpu.make_async_copy(ref, ref, sem).wait()


def reduce_phases(here, rows, width, produce, finish, part, buffers, sems):
    in1, in2, in3, in4 = buffers
    sent, sem1, sem2, sem3, sem4 = sems
    side, depth = here.side, here.depth
    tall = depth * rows
    cuts = slices_of(width)

    def rows_of(z):
        return pl.ds(pl.multiple_of(z * rows, rows), rows)

    every = slice(None)

    def core_copy(s):
        cols = pl.ds(*cuts[s])
        return remote(
            part(every, every, 1 - here.core, cols),
            in1.at[:, :, :, cols],
            sent.at[0],
            sem1.at[s],
            here.at(flip=True),
        )

    def offsets(s, a, b):
        return (a, b) if s % 2 == 0 else (b, a)

    def first_copy(s, ja, kb, sending):
        cols = pl.ds(*cuts[s])
        slot = side - ja - 1
        y, x = here.line(*offsets(s, ja, kb))
        return remote(
            in1.at[y, x, :, cols],
            in2.at[slot, kb, :, cols],
            sent.at[1],
            sem2.at[s, (side - ja if sending else ja) - 1, kb],
            here.at(*offsets(s, ja, 0)),
        )

    def second_copy(s, kb, sending):
        cols = pl.ds(*cuts[s])
        y, x = here.line(*offsets(s, 0, kb))
        return remote(
            in1.at[y, x, :, cols],
            in3.at[side - kb - 1, :, cols],
            sent.at[2],
            sem3.at[s, (side - kb if sending else kb) - 1],
            here.at(*offsets(s, 0, kb)),
        )

    def depth_copy(s, jz):
        cols = pl.ds(*cuts[s])
        return remote(
            in1.at[here.y, here.x, rows_of(lax.rem(here.z + jz, depth)), cols],
            in4.at[depth - jz - 1, :, cols],
            sent.at[3],
            sem4.at[s],
            here.at(0, 0, jz),
        )

    def phase0(s):
        cols = pl.ds(*cuts[s])
        value = produce(s, cols).astype(jnp.bfloat16).reshape(side, side, 2, tall, cuts[s][1])
        for core in range(2):
            part(every, every, core, cols)[...] = value[:, :, core]
        core_copy(s).start()

    def phase1(s):
        cols = pl.ds(*cuts[s])
        core_copy(s).wait_recv()
        for a in list(range(1, side)) + [0]:
            for b in list(range(1, side)) + [0]:
                y, x = here.line(*offsets(s, a, b))
                total = wide(part(y, x, here.core, cols)[...]) + wide(in1[y, x, :, cols])
                in1[y, x, :, cols] = total.astype(jnp.bfloat16)
                if a:
                    first_copy(s, a, b, True).start()

    def phase2(s):
        cols = pl.ds(*cuts[s])
        for b in list(range(1, side)) + [0]:
            y, x = here.line(*offsets(s, 0, b))
            total = wide(in1[y, x, :, cols])
            for a in range(1, side):
                first_copy(s, a, b, False).wait_recv()
                total = total + wide(in2[a - 1, b, :, cols])
            in1[y, x, :, cols] = total.astype(jnp.bfloat16)
            if b:
                second_copy(s, b, True).start()

    def phase3(s):
        cols = pl.ds(*cuts[s])
        total = wide(in1[here.y, here.x, :, cols])
        for b in range(1, side):
            second_copy(s, b, False).wait_recv()
            total = total + wide(in3[b - 1, :, cols])
        if depth == 1:
            finish(s, cols, total)
            return
        in1[here.y, here.x, :, cols] = total.astype(jnp.bfloat16)
        for jz in range(1, depth):
            depth_copy(s, jz).start()

    def phase4(s):
        cols = pl.ds(*cuts[s])
        total = wide(in1[here.y, here.x, rows_of(here.z), cols])
        wait_bytes(in4.at[:, :, cols], sem4.at[s])
        for jz in range(1, depth):
            total = total + wide(in4[jz - 1, :, cols])
        finish(s, cols, total)

    def wait_core():
        wait_bytes(in1, sent.at[0])

    def wait_sent():
        wait_bytes(in1.at[0 : side - 1], sent.at[1])
        wait_bytes(in1.at[0, 0 : side - 1], sent.at[2])
        if depth > 1:
            wait_bytes(in1.at[0, 0, 0 : (depth - 1) * rows, :], sent.at[3])

    phases = phase0, phase1, phase2, phase3, phase4
    return phases[: 4 if depth == 1 else 5], wait_core, wait_sent


def gather_phases(here, held, rows, features, consume, sems):
    side, depth = here.side, here.depth
    sent, zsem, lsem, csem = sems
    cuts = slices_of(features)
    cuts[-1] = (cuts[-1][0], held.shape[-1] - cuts[-1][0])

    def rows_of(z):
        return pl.ds(pl.multiple_of(z * rows, rows), rows)

    def line_ref(s, ky, kx, core):
        y, x = here.line(ky, kx)
        return held.at[y, x, core, :, pl.ds(*cuts[s])]

    def arrival(s, ky, kx):
        return lsem.at[s, (ky % side) * side + kx % side - 1]

    def own_send(s, jz):
        ref = held.at[here.y, here.x, here.core, rows_of(lax.rem(here.z + jz, depth)), pl.ds(*cuts[s])]
        for j in range(1, side):
            for jy, jx in ((j, 0), (0, j)) if s % 2 == 0 else ((0, j), (j, 0)):
                remote(ref, ref, sent.at[1], arrival(s, -jy, -jx), here.at(jy, jx)).start()

    def core_send(s, ky, kx):
        ref = line_ref(s, ky, kx, here.core)
        remote(ref, ref, sent.at[3], csem.at[s], here.at(flip=True)).start()

    def plane_wait(s, ky, kx):
        wait_bytes(line_ref(s, ky, kx, here.core), arrival(s, ky, kx))

    def turn(s, a, b):
        return (a, b) if s % 2 == 0 else (b, a)

    def phase0(s):
        ref = held.at[here.y, here.x, here.core, rows_of(here.z), pl.ds(*cuts[s])]
        for j in range(1, depth):
            remote(ref, ref, sent.at[0], zsem.at[s], here.at(0, 0, j)).start()
        own_send(s, 0)

    def phase1(s):
        others = held.at[here.y, here.x, here.core, 0 : (depth - 1) * rows, pl.ds(*cuts[s])]
        wait_bytes(others, zsem.at[s])
        for j in range(1, depth):
            own_send(s, j)
        core_send(s, 0, 0)

    def phase2(s):
        for k in range(1, side):
            plane_wait(s, *turn(s, k, 0))
            ref = line_ref(s, *turn(s, k, 0), here.core)
            for j in range(1, side):
                jy, jx = turn(s, 0, j)
                ky, kx = turn(s, k, 0)
                remote(ref, ref, sent.at[2], arrival(s, ky - jy, kx - jx), here.at(jy, jx)).start()
            core_send(s, *turn(s, k, 0))

    def phase3(s):
        for b in range(1, side):
            for a in range(side):
                plane_wait(s, *turn(s, a, b))
                core_send(s, *turn(s, a, b))

    def phase4(s):
        wait_bytes(held.at[:, :, 1 - here.core, :, pl.ds(*cuts[s])], csem.at[s])
        consume(s)

    def wait_sent():
        if depth > 1:
            wait_bytes(held.at[0, 0, 0, 0 : (depth - 1) * rows, :], sent.at[0])
        wait_bytes(held.at[0 : side - 1, 0:2, 0], sent.at[1])
        wait_bytes(held.at[0 : side - 1, 0 : side - 1, 0], sent.at[2])
        wait_bytes(held.at[:, :, 0], sent.at[3])

    return (phase0, phase1, phase2, phase3, phase4), wait_sent


def run_in_order(groups):
    tasks = []
    for phases, count, keys in groups:
        last = [-1.0] * count
        for phase, (start, burst, quick, pace) in zip(phases, keys):
            for s in range(count):
                last[s] = max(last[s] + 1e-6, start + quick * min(s, burst) + pace * max(0, s - burst))
                tasks.append((last[s], len(tasks), phase, s))
    for _, _, phase, s in sorted(tasks, key=lambda task: task[:2]):
        phase(s)


def layer_kernel(
    side, depth, lengths, queries, new_keys, new_values, resid, gain, router, named_ids,
    keys_hbm, values_hbm, proj_hbm, gate_hbm, up_hbm, down_hbm, mixed,
    keys, values, query_rows, blend_rows, attended,
    proj, gate, up, down, regrouped, hidden, held, act, gate_sum, up_sum,
    ksem, wsem, xsem, *scratch
):
    here, flat = Place(side, depth), Place(side, 1)
    rows, features = resid.shape
    experts = router.shape[0]
    count = 2 * side * side
    width = attended.shape[1] // count
    span = keys_hbm.shape[1]
    group_size = H // KVH
    pieces = count // KVH
    own_group = here.ep // pieces

    def peer(j):
        return lax.rem(here.ep + j, count)

    peers = [(peer(j), here.z) for j in range(1, count)] + [here.at(0, 0, j) for j in range(1, depth)]
    announce(peers)

    def turn_group(i):
        return lax.rem(own_group + 1 + i, KVH)

    def lanes(g):
        return pl.ds(pl.multiple_of(g * HD, HD), HD)

    def cache_copies(i):
        return [
            pltpu.make_async_copy(
                src.at[:, :, lanes(turn_group(i))], dst.at[:, 0:span, lanes(turn_group(i))], ksem.at[n, i]
            )
            for n, (src, dst) in enumerate(((keys_hbm, keys), (values_hbm, values)))
        ]

    for i in range(KVH):
        for copy in cache_copies(i):
            copy.start()
    loads = [
        pltpu.make_async_copy(src, dst, wsem.at[i])
        for i, (src, dst) in enumerate(
            ((proj_hbm, proj), (gate_hbm.at[0], gate), (up_hbm.at[0], up), (down_hbm.at[0], down))
        )
    ]
    loads[0].start()

    first = lax.broadcasted_iota(jnp.int32, (PAD, KVH * HD), 0) == 0
    for new, cache in ((new_keys, keys), (new_values, values)):
        wide_new = new[...].astype(jnp.float32)
        for token in range(rows):
            own = jnp.where(first, wide_new[token : token + 1, :], 0.0)
            cache[token, span:, :] = own.astype(jnp.bfloat16)

    def piece(index):
        return attended.at[:, pl.ds(pl.multiple_of(index * width, 128), width)]

    def exchange(to, source):
        return remote(piece(to), regrouped.at[source], xsem.at[0], xsem.at[1], (to, here.z))

    def attend(i):
        g = turn_group(i)
        for copy in cache_copies(i):
            copy.wait()
        for h in range(group_size):
            query_rows[h * rows : (h + 1) * rows, :] = wide(queries[:, lanes(g * group_size + h)])
        scores = []
        place = lax.broadcasted_iota(jnp.int32, (group_size, span + PAD), 1)
        for token in range(rows):
            query = query_rows[pl.ds(token, group_size, stride=rows), :]
            score = nt_dot(query.astype(jnp.bfloat16), keys[token, :, lanes(g)])
            kept = (place < lengths[token]) | (place == span)
            scores.append(jnp.where(kept, score * (1.0 / math.sqrt(HD)), -1e30))
        score = jnp.concatenate(scores, axis=0)
        grown = jnp.exp(score - jnp.max(score, axis=1, keepdims=True))
        weights = (grown / jnp.sum(grown, axis=1, keepdims=True)).astype(jnp.bfloat16)
        for token in range(rows):
            blend_rows[pl.ds(token, group_size, stride=rows), :] = jnp.dot(
                weights[token * group_size : (token + 1) * group_size, :],
                values[token, :, lanes(g)],
                preferred_element_type=jnp.float32,
            )
        for h in range(group_size):
            attended[:, lanes(g * group_size + h)] = blend_rows[h * rows : (h + 1) * rows, :].astype(
                jnp.bfloat16
            )

    for i in range(KVH):
        if i == KVH - 1:
            gathered(peers)
            for load in loads[1:]:
                load.start()
            for sent in range(i):
                for k in range(pieces):
                    exchange(turn_group(sent) * pieces + k, here.ep).start()
        attend(i)
    for k in range(1, pieces):
        exchange(own_group * pieces + lax.rem(here.ep + k, pieces), here.ep).start()
    regrouped[here.ep] = attended[:, pl.ds(pl.multiple_of(here.ep * width, 128), width)]

    eye = jnp.where(
        lax.broadcasted_iota(jnp.int32, (rows, rows), 0) == lax.broadcasted_iota(jnp.int32, (rows, rows), 1), 1.0, 0.0
    ).astype(jnp.bfloat16)
    label = lax.broadcasted_iota(jnp.int32, (experts, rows), 0)
    hits = jnp.zeros((experts, rows), jnp.float32)
    for k in range(TOP):
        hits = hits + jnp.where(label == named_ids[k : k + 1, :], 1.0, 0.0)
    named = nt_dot(eye, hits.astype(jnp.bfloat16)) > 0.5

    loads[0].wait()
    with jax.named_scope("exchange_wait"):
        wait_bytes(regrouped.at[0 : count - 1], xsem.at[1])

    def produce_proj(s, cols):
        left = regrouped[...].reshape(count * rows, width)
        return jnp.dot(left, proj[:, cols], preferred_element_type=jnp.float32)

    squares, logits = [], []
    slices = len(slices_of(features))
    tail_width = held.shape[-1] - features
    mine = pl.ds(pl.multiple_of(here.z * rows, rows), rows)

    def finish_proj(s, cols, total):
        value = resid[:, cols].astype(jnp.float32) + total
        hidden[:, cols] = value
        scaled = (value * gain[:, cols]).astype(jnp.bfloat16)
        held[here.y, here.x, here.core, mine, cols] = scaled
        if s < slices - 1:
            gather[0](s)
        squares.append(jnp.sum(value * value, axis=1, keepdims=True))
        logits.append(nt_dot(scaled, router[:, cols]))
        if s == slices - 1:
            scale = lax.rsqrt(jnp.maximum(sum(squares) / features, 0.25))
            scores = sum(logits) * scale
            peak = jnp.max(jnp.where(named, scores, -jnp.inf), axis=1, keepdims=True)
            grown = jnp.where(named, jnp.exp(jnp.where(named, scores - peak, 0.0)), 0.0)
            probs = grown / jnp.sum(grown, axis=1, keepdims=True)
            high = scale.astype(jnp.bfloat16).astype(jnp.float32)
            lane = lax.broadcasted_iota(jnp.int32, (rows, tail_width), 1)
            tail = jnp.where(lane == experts, high, jnp.where(lane == experts + 1, scale - high, 0.0))
            held[here.y, here.x, here.core, mine, features:] = tail.astype(jnp.bfloat16)
            held[here.y, here.x, here.core, mine, features : features + experts] = probs.astype(jnp.bfloat16)
            gather[0](s)

    group = side * 2 * depth * rows

    def rows_at(y):
        return pl.ds(pl.multiple_of(y * group, group), group)

    def consume(s):
        if s == 0:
            loads[1].wait()
            loads[2].wait()
        start, size = slices_of(features)[s]

        def step(y, carry):
            block = held[y, :, :, :, start : start + size].reshape(group, size)
            for weight, total in ((gate, gate_sum), (up, up_sum)):
                value = jnp.dot(
                    block, weight[start : start + size, :], preferred_element_type=jnp.float32
                )
                total[rows_at(y), :] = value if s == 0 else total[rows_at(y), :] + value
            return carry

        lax.fori_loop(0, side, step, 0)

    proj_buffers, expert_buffers, rest = scratch[:4], scratch[4:8], scratch[8:]
    proj_sems, expert_sems, gather_sems = rest[:5], rest[5:10], rest[10:]
    def rows_of(block):
        return pl.ds(block * rows if isinstance(block, int) else pl.multiple_of(block * rows, rows), rows)

    def proj_parts(y, x, core, cols):
        return expert_buffers[0].at[y, x, rows_of(core), cols]

    reduce, wait_core, wait_reduce = reduce_phases(
        flat, rows, features, produce_proj, finish_proj, proj_parts, proj_buffers, proj_sems
    )
    gather, wait_gather = gather_phases(here, held, rows, features, consume, gather_sems)

    def finish_core(s):
        wait_core()

    run_in_order(
        (
            (reduce, slices, PROJ_KEYS),
            ((finish_core,), 1, (PROJ_KEYS[3],)),
            (gather[1:], slices, GATHER_KEYS),
        )
    )
    loads[3].wait()
    with jax.named_scope("drain_gather"):
        wait_reduce()
        wait_gather()
        wait_bytes(regrouped.at[0 : count - 1], xsem.at[0])
    expert = (here.ep * depth + here.z) // 2

    def activate(y, carry):
        tail = held[y, :, :, :, features:].reshape(group, tail_width).astype(jnp.float32)
        lane = lax.broadcasted_iota(jnp.int32, tail.shape, 1)
        weight = jnp.sum(jnp.where(lane == expert, tail, 0.0), axis=1, keepdims=True)
        scale = jnp.sum(
            jnp.where((lane == experts) | (lane == experts + 1), tail, 0.0), axis=1, keepdims=True
        )
        gate_val = gate_sum[rows_at(y), :] * scale
        value = gate_val / (1.0 + jnp.exp(-gate_val)) * (up_sum[rows_at(y), :] * (scale * weight))
        act[rows_at(y), :] = value.astype(jnp.bfloat16)
        return carry

    lax.fori_loop(0, side, activate, 0)

    def produce(s, cols):
        return jnp.dot(act[...], down[:, cols], preferred_element_type=jnp.float32)

    def finish(s, cols, total):
        mixed[:, cols] = hidden[:, cols] + total

    def parts(y, x, core, cols):
        return held.at[y, x, core, :, cols]

    spread, wait_core, wait_spread = reduce_phases(
        here, rows, features, produce, finish, parts, expert_buffers, expert_sems
    )
    run_in_order(((spread, slices, SPREAD_KEYS),))
    with jax.named_scope("drain_spread"):
        wait_core()
        wait_spread()


PROJ_KEYS = ((0.0, 0, 0.0, 0.3), (1.3, 0, 0.0, 0.3), (4.4, 0, 0.0, 0.4), (7.2, 0, 0.0, 0.4))
GATHER_KEYS = ((12.0, 0, 0.0, 1.2), (15.0, 0, 0.0, 1.5), (18.0, 0, 0.0, 1.75), (21.0, 0, 0.0, 1.75))
SPREAD_KEYS = ((0.0, 0, 0.0, 0.45), (1.0, 4, 0.5, 1.75), (5.5, 0, 0.0, 1.75), (9.0, 0, 0.0, 1.75), (14.5, 0, 0.0, 1.75))


def nt_dot(left, right):
    return lax.dot_general(left, right, (((1,), (1,)), ((), ())), preferred_element_type=jnp.float32)


PAD = 16


def run_layer(
    side, depth, lengths, queries, new_keys, new_values, resid, gain, router, named_ids,
    cache_keys, cache_values, out_proj, gate_slab, up_slab, down_slab
):
    rows, width = resid.shape
    n = len(slices_of(width))
    experts = router.shape[0]
    span = cache_keys.shape[1]
    bf, dma = jnp.bfloat16, pltpu.SemaphoreType.DMA
    plane = 2 * side * side
    count = plane * depth
    tail = pl.cdiv(experts + 2, 128) * 128
    vmem, anywhere = pl.BlockSpec(memory_space=pltpu.VMEM), pl.BlockSpec(memory_space=pl.ANY)
    return pl.pallas_call(
        lambda *refs: layer_kernel(side, depth, *refs),
        out_shape=jax.ShapeDtypeStruct((rows, width), jnp.float32),
        in_specs=[pl.BlockSpec(memory_space=pltpu.SMEM)] + [vmem] * 7 + [anywhere] * 6,
        out_specs=vmem,
        scratch_shapes=[
            pltpu.VMEM((rows, span + PAD, KVH * HD), bf),
            pltpu.VMEM((rows, span + PAD, KVH * HD), bf),
            pltpu.VMEM((H // KVH * rows, HD), jnp.float32),
            pltpu.VMEM((H // KVH * rows, HD), jnp.float32),
            pltpu.VMEM((rows, H * HD), bf),
            pltpu.VMEM(out_proj.shape, bf),
            pltpu.VMEM(gate_slab.shape[1:], bf),
            pltpu.VMEM(up_slab.shape[1:], bf),
            pltpu.VMEM(down_slab.shape[1:], bf),
            pltpu.VMEM((plane, rows, H * HD // plane), bf),
            pltpu.VMEM((rows, width), jnp.float32),
            pltpu.VMEM((side, side, 2, depth * rows, width + tail), bf),
            pltpu.VMEM((count * rows, gate_slab.shape[2]), bf),
            pltpu.VMEM((count * rows, gate_slab.shape[2]), jnp.float32),
            pltpu.VMEM((count * rows, gate_slab.shape[2]), jnp.float32),
            dma((2, KVH)),
            dma((4,)),
            dma((2,)),
        ]
        + reduce_shapes(side, 1, rows, width)
        + reduce_shapes(side, depth, rows, width)
        + reduce_sems(side, n) * 2
        + [dma((4,)), dma((n,)), dma((n, side * side - 1)), dma((n,))],
        compiler_params=pltpu.CompilerParams(
            collective_id=0, has_side_effects=True, vmem_limit_bytes=VMEM_LIMIT
        ),
    )(
        lengths, queries, new_keys, new_values, resid, gain, router, named_ids,
        cache_keys, cache_values, out_proj, gate_slab, up_slab, down_slab,
    )


def local(
    resid,
    queries,
    new_keys,
    new_values,
    cache_keys,
    cache_values,
    cache_len,
    out_proj,
    norm_gain,
    router,
    expert_ids,
    gate_slab,
    up_slab,
    down_slab,
):
    side = math.isqrt(lax.axis_size("ep") // 2)
    depth = lax.axis_size("dp")
    return run_layer(
        side, depth, cache_len, queries, new_keys, new_values, resid, norm_gain.reshape(1, -1),
        router.T, expert_ids.T, cache_keys, cache_values, out_proj, gate_slab, up_slab, down_slab,
    )


def solution(mesh):
    in_specs = (
        P(("ep", "dp"), None),
        P(("ep", "dp"), None),
        P(("ep", "dp"), None),
        P(("ep", "dp"), None),
        P(("ep", "dp"), None, None),
        P(("ep", "dp"), None, None),
        P(("ep", "dp")),
        P("ep", None),
        P(),
        P(),
        P(("ep", "dp"), None),
        P(("ep", "dp"), None, None),
        P(("ep", "dp"), None, None),
        P(("ep", "dp"), None, None),
    )
    out_specs = P(("ep", "dp"), None)
    return jax.shard_map(local, mesh=mesh, in_specs=in_specs, out_specs=out_specs, check_vma=False)
```

```python
import math

import jax
import jax.numpy as jnp
from jax import lax
from jax.experimental import pallas as pl
from jax.experimental.pallas import tpu as pltpu
from jax.sharding import PartitionSpec as P

D = 4096
H = 64
KVH = 4
HD = 128
TOP = 8


MESH = pl.DeviceIdType.MESH
VMEM_LIMIT = 67_000_000


class Place:
    def __init__(self, side, depth):
        self.side, self.depth = side, depth
        ep = lax.axis_index("ep")
        self.ep = ep
        self.core = lax.rem(ep, 2)
        self.x = lax.rem(ep // 2, side)
        self.y = ep // (2 * side)
        self.z = lax.axis_index("dp")

    def at(self, dy=0, dx=0, dz=0, flip=False):
        y, x = self.line(dy, dx)
        z = lax.rem(self.z + dz, self.depth) if dz else self.z
        core = 1 - self.core if flip else self.core
        return ((y * self.side + x) * 2 + core, z)

    def line(self, dy, dx):
        return lax.rem(self.y + dy, self.side), lax.rem(self.x + dx, self.side)


def announce(devices):
    barrier = pltpu.get_barrier_semaphore()
    for device in devices:
        pl.semaphore_signal(barrier, inc=1, device_id=device, device_id_type=MESH)


def gathered(devices):
    pl.semaphore_wait(pltpu.get_barrier_semaphore(), len(devices))


def remote(src, dst, send, recv, device):
    return pltpu.make_async_remote_copy(
        src_ref=src, dst_ref=dst, send_sem=send, recv_sem=recv, device_id=device, device_id_type=MESH
    )


SLICE = 512
STAGES = 8
ORDER = (
    3, 2, 4, 5, 11, 0, 10, 1, 7, 12, 9, 8, 6, 15, 19, 13, 20, 14, 18, 16,
    17, 27, 23, 28, 21, 22, 25, 24, 26, 30, 29, 36, 31, 32, 35, 33, 34, 59, 38, 60,
    40, 39, 44, 43, 57, 37, 56, 42, 58, 51, 68, 48, 47, 62, 46, 67, 65, 52, 61, 41,
    54, 55, 63, 45, 64, 50, 53, 70, 49, 75, 66, 89, 76, 95, 69, 94, 73, 71, 90, 83,
    93, 72, 81, 78, 84, 103, 98, 97, 74, 80, 77, 86, 79, 82, 85, 87, 124, 123, 120, 127,
    132, 131, 128, 125, 135, 126, 88, 121, 92, 134, 140, 129, 122, 139, 143, 136, 130, 91, 100, 148,
    142, 133, 106, 147, 137, 151, 101, 144, 102, 105, 138, 96, 99, 150, 108, 141, 145, 110, 146, 149,
    114, 107, 159, 111, 109, 104, 116, 155, 112, 154, 153, 115, 113, 117, 152, 118, 119, 158, 156, 157,
)


def slices_of(width):
    return [(start, SLICE) for start in range(0, width, SLICE)]


def task_order(count):
    if count == STAGES:
        return [(code // STAGES, code % STAGES) for code in ORDER]
    return [(task, s) for task in range(20) for s in range(count)]


def reduce_shapes(side, depth, rows, width):
    bf = jnp.bfloat16
    return [
        pltpu.VMEM((depth, side, side, rows, width), bf),
        pltpu.VMEM((depth, side - 1, side, rows, width), bf),
        pltpu.VMEM((depth, side - 1, rows, width), bf),
    ]


def reduce_sems(side, n):
    dma = pltpu.SemaphoreType.DMA
    return [dma((3,)), dma((n,)), dma((n, side - 1, side)), dma((n, side - 1))]


def wide(value):
    return value.astype(jnp.float32)


def wait_bytes(ref, sem):
    pltpu.make_async_copy(ref, ref, sem).wait()


def reduce_phases(here, group, rows, width, produce, finish, part, buffers, sems):
    in1, in2, in3 = buffers
    sent, sem1, sem2, sem3 = sems
    side = here.side
    cuts = slices_of(width)
    every = slice(None)

    def core_copy(s):
        cols = pl.ds(*cuts[s])
        return remote(
            part(every, every, 1 - here.core, cols),
            in1.at[group, :, :, :, cols],
            sent.at[0],
            sem1.at[s],
            here.at(flip=True),
        )

    def offsets(s, a, b):
        return (a, b) if s % 2 == 0 else (b, a)

    def first_copy(s, ja, kb, sending):
        cols = pl.ds(*cuts[s])
        slot = side - ja - 1
        y, x = here.line(*offsets(s, ja, kb))
        return remote(
            in1.at[group, y, x, :, cols],
            in2.at[group, slot, kb, :, cols],
            sent.at[1],
            sem2.at[s, (side - ja if sending else ja) - 1, kb],
            here.at(*offsets(s, ja, 0)),
        )

    def second_copy(s, kb, sending):
        cols = pl.ds(*cuts[s])
        y, x = here.line(*offsets(s, 0, kb))
        return remote(
            in1.at[group, y, x, :, cols],
            in3.at[group, side - kb - 1, :, cols],
            sent.at[2],
            sem3.at[s, (side - kb if sending else kb) - 1],
            here.at(*offsets(s, 0, kb)),
        )

    def phase0(s):
        cols = pl.ds(*cuts[s])

        def put(value, place):
            value = value.astype(jnp.bfloat16).reshape(-1, side, side, 2, rows, cuts[s][1])
            for core in range(2):
                part(every, every, core, cols, place)[...] = value[:, :, :, core]

        produce(s, cols, put)
        core_copy(s).start()

    def phase1(s):
        cols = pl.ds(*cuts[s])
        core_copy(s).wait_recv()
        for a in list(range(1, side)) + [0]:
            for b in list(range(1, side)) + [0]:
                y, x = here.line(*offsets(s, a, b))
                total = wide(part(y, x, here.core, cols)[...]) + wide(in1[group, y, x, :, cols])
                in1[group, y, x, :, cols] = total.astype(jnp.bfloat16)
                if a:
                    first_copy(s, a, b, True).start()

    def phase2(s):
        cols = pl.ds(*cuts[s])
        for b in list(range(1, side)) + [0]:
            y, x = here.line(*offsets(s, 0, b))
            total = wide(in1[group, y, x, :, cols])
            for a in range(1, side):
                first_copy(s, a, b, False).wait_recv()
                total = total + wide(in2[group, a - 1, b, :, cols])
            in1[group, y, x, :, cols] = total.astype(jnp.bfloat16)
            if b:
                second_copy(s, b, True).start()

    def phase3(s):
        cols = pl.ds(*cuts[s])
        total = wide(in1[group, here.y, here.x, :, cols])
        for b in range(1, side):
            second_copy(s, b, False).wait_recv()
            total = total + wide(in3[group, b - 1, :, cols])
        finish(s, cols, total)

    def wait_core():
        wait_bytes(in1.at[group], sent.at[0])

    def wait_sent():
        wait_bytes(in1.at[group, 0 : side - 1], sent.at[1])
        wait_bytes(in1.at[group, 0, 0 : side - 1], sent.at[2])

    return (phase0, phase1, phase2, phase3), wait_core, wait_sent


def gather_phases(here, held, group, features, sems):
    side = here.side
    sent, lsem, csem = sems
    cuts = slices_of(features)
    cuts[-1] = (cuts[-1][0], held.shape[-1] - cuts[-1][0])

    def line_ref(s, ky, kx, core):
        y, x = here.line(ky, kx)
        return held.at[group, y, x, core, :, pl.ds(*cuts[s])]

    def arrival(s, ky, kx):
        return lsem.at[s, (ky % side) * side + kx % side - 1]

    def core_send(s, ky, kx):
        ref = line_ref(s, ky, kx, here.core)
        remote(ref, ref, sent.at[2], csem.at[s], here.at(flip=True)).start()

    def plane_wait(s, ky, kx):
        wait_bytes(line_ref(s, ky, kx, here.core), arrival(s, ky, kx))

    def turn(s, a, b):
        return (a, b) if s % 2 == 0 else (b, a)

    def own_send(s):
        ref = line_ref(s, 0, 0, here.core)
        for j in range(1, side):
            for jy, jx in (turn(s, j, 0), turn(s, 0, j)):
                remote(ref, ref, sent.at[0], arrival(s, -jy, -jx), here.at(jy, jx)).start()
        core_send(s, 0, 0)

    def forward(s):
        for k in range(1, side):
            plane_wait(s, *turn(s, k, 0))
            ref = line_ref(s, *turn(s, k, 0), here.core)
            for j in range(1, side):
                jy, jx = turn(s, 0, j)
                ky, kx = turn(s, k, 0)
                remote(ref, ref, sent.at[1], arrival(s, ky - jy, kx - jx), here.at(jy, jx)).start()
            core_send(s, *turn(s, k, 0))

    def collect(s):
        for b in range(1, side):
            for a in range(side):
                plane_wait(s, *turn(s, a, b))
                core_send(s, *turn(s, a, b))

    def arrive(s):
        wait_bytes(held.at[group, :, :, 1 - here.core, :, pl.ds(*cuts[s])], csem.at[s])

    def wait_sent():
        wait_bytes(held.at[group, 0 : side - 1, 0:2, 0], sent.at[0])
        wait_bytes(held.at[group, 0 : side - 1, 0 : side - 1, 0], sent.at[1])
        wait_bytes(held.at[group, :, :, 0], sent.at[2])

    return (own_send, forward, collect, arrive), wait_sent


def layer_kernel(
    side, depth, lengths, queries, new_keys, new_values, resid, gain, router, named_ids,
    keys_hbm, values_hbm, proj_hbm, gate_hbm, up_hbm, down_hbm, mixed,
    keys, values, query_rows, blend_rows, attended,
    proj, gate, up, down, regrouped, hidden, held, act, gate_sum, up_sum,
    ksem, wsem, xsem, zsem, zsent, *scratch
):
    here, flat = Place(side, depth), Place(side, 1)
    rows, features = resid.shape
    experts = router.shape[0]
    count = 2 * side * side
    width = attended.shape[1] // count
    span = keys_hbm.shape[1]
    group_size = H // KVH
    pieces = count // KVH
    own_group = here.ep // pieces

    def peer(j):
        return lax.rem(here.ep + j, count)

    peers = [(peer(j), here.z) for j in range(1, count)] + [here.at(0, 0, j) for j in range(1, depth)]
    announce(peers)

    def turn_group(i):
        return lax.rem(own_group + 1 + i, KVH)

    def lanes(g):
        return pl.ds(pl.multiple_of(g * HD, HD), HD)

    def cache_copies(i):
        return [
            pltpu.make_async_copy(
                src.at[:, :, lanes(turn_group(i))], dst.at[:, 0:span, lanes(turn_group(i))], ksem.at[n, i]
            )
            for n, (src, dst) in enumerate(((keys_hbm, keys), (values_hbm, values)))
        ]

    for i in range(KVH):
        for copy in cache_copies(i):
            copy.start()
    loads = [
        pltpu.make_async_copy(src, dst, wsem.at[i])
        for i, (src, dst) in enumerate(
            ((proj_hbm, proj), (gate_hbm.at[0], gate), (up_hbm.at[0], up), (down_hbm.at[0], down))
        )
    ]
    loads[0].start()

    first = lax.broadcasted_iota(jnp.int32, (PAD, KVH * HD), 0) == 0
    for new, cache in ((new_keys, keys), (new_values, values)):
        wide_new = new[...].astype(jnp.float32)
        for token in range(rows):
            own = jnp.where(first, wide_new[token : token + 1, :], 0.0)
            cache[token, span:, :] = own.astype(jnp.bfloat16)

    def piece(index):
        return attended.at[:, pl.ds(pl.multiple_of(index * width, 128), width)]

    def exchange(to, source):
        return remote(piece(to), regrouped.at[source], xsem.at[0], xsem.at[1], (to, here.z))

    def attend(i):
        g = turn_group(i)
        for copy in cache_copies(i):
            copy.wait()
        for h in range(group_size):
            query_rows[h * rows : (h + 1) * rows, :] = wide(queries[:, lanes(g * group_size + h)])
        scores = []
        place = lax.broadcasted_iota(jnp.int32, (group_size, span + PAD), 1)
        for token in range(rows):
            query = query_rows[pl.ds(token, group_size, stride=rows), :]
            score = nt_dot(query.astype(jnp.bfloat16), keys[token, :, lanes(g)])
            kept = (place < lengths[token]) | (place == span)
            scores.append(jnp.where(kept, score * (1.0 / math.sqrt(HD)), -1e30))
        score = jnp.concatenate(scores, axis=0)
        grown = jnp.exp(score - jnp.max(score, axis=1, keepdims=True))
        weights = (grown / jnp.sum(grown, axis=1, keepdims=True)).astype(jnp.bfloat16)
        for token in range(rows):
            blend_rows[pl.ds(token, group_size, stride=rows), :] = jnp.dot(
                weights[token * group_size : (token + 1) * group_size, :],
                values[token, :, lanes(g)],
                preferred_element_type=jnp.float32,
            )
        for h in range(group_size):
            attended[:, lanes(g * group_size + h)] = blend_rows[h * rows : (h + 1) * rows, :].astype(
                jnp.bfloat16
            )

    for i in range(KVH):
        if i == KVH - 1:
            gathered(peers)
            for load in loads[1:]:
                load.start()
            for sent in range(i):
                for k in range(pieces):
                    exchange(turn_group(sent) * pieces + k, here.ep).start()
        attend(i)
    for k in range(1, pieces):
        exchange(own_group * pieces + lax.rem(here.ep + k, pieces), here.ep).start()
    regrouped[here.ep] = attended[:, pl.ds(pl.multiple_of(here.ep * width, 128), width)]

    eye = jnp.where(
        lax.broadcasted_iota(jnp.int32, (rows, rows), 0) == lax.broadcasted_iota(jnp.int32, (rows, rows), 1), 1.0, 0.0
    ).astype(jnp.bfloat16)
    label = lax.broadcasted_iota(jnp.int32, (experts, rows), 0)
    hits = jnp.zeros((experts, rows), jnp.float32)
    for k in range(TOP):
        hits = hits + jnp.where(label == named_ids[k : k + 1, :], 1.0, 0.0)
    named = nt_dot(eye, hits.astype(jnp.bfloat16)) > 0.5

    loads[0].wait()
    with jax.named_scope("exchange_wait"):
        wait_bytes(regrouped.at[0 : count - 1], xsem.at[1])

    def produce_proj(s, cols, put):
        left = regrouped[...].reshape(count * rows, width)
        put(jnp.dot(left, proj[:, cols], preferred_element_type=jnp.float32), None)

    squares, logits = [], []
    slices = len(slices_of(features))
    tail_width = held.shape[-1] - features

    def finish_proj(s, cols, total):
        value = resid[:, cols].astype(jnp.float32) + total
        hidden[:, cols] = value
        scaled = (value * gain[:, cols]).astype(jnp.bfloat16)
        held[0, here.y, here.x, here.core, :, cols] = scaled
        if s < slices - 1:
            launch(s)
        squares.append(jnp.sum(value * value, axis=1, keepdims=True))
        logits.append(nt_dot(scaled, router[:, cols]))
        if s == slices - 1:
            scale = lax.rsqrt(jnp.maximum(sum(squares) / features, 0.25))
            scores = sum(logits) * scale
            peak = jnp.max(jnp.where(named, scores, -jnp.inf), axis=1, keepdims=True)
            grown = jnp.where(named, jnp.exp(jnp.where(named, scores - peak, 0.0)), 0.0)
            probs = grown / jnp.sum(grown, axis=1, keepdims=True)
            high = scale.astype(jnp.bfloat16).astype(jnp.float32)
            lane = lax.broadcasted_iota(jnp.int32, (rows, tail_width), 1)
            tail = jnp.where(lane == experts, high, jnp.where(lane == experts + 1, scale - high, 0.0))
            held[0, here.y, here.x, here.core, :, features:] = tail.astype(jnp.bfloat16)
            held[0, here.y, here.x, here.core, :, features : features + experts] = probs.astype(jnp.bfloat16)
            launch(s)

    near, far = slice(0, 1), slice(1, depth)
    plane_rows = count * rows

    def launch(s):
        start, size = slices_of(features)[s]
        cols = pl.ds(start, size if s < slices - 1 else held.shape[-1] - start)
        for j in range(1, depth):
            remote(
                held.at[0, here.y, here.x, here.core, :, cols],
                held.at[depth - j, here.y, here.x, here.core, :, cols],
                zsent.at[0],
                zsem.at[s],
                here.at(0, 0, j),
            ).start()
        near_gather[0](s)

    def relay(s):
        start, size = slices_of(features)[s]
        cols = pl.ds(start, size if s < slices - 1 else held.shape[-1] - start)
        wait_bytes(held.at[far, here.y, here.x, here.core, :, cols], zsem.at[s])
        far_gather[0](s)

    def over(group, body):
        height = plane_rows * (group.stop - group.start)
        if height <= 512:
            body(group, pl.ds(group.start * plane_rows, height))
            return

        def step(j, carry):
            body(pl.ds(j, 1), pl.ds(pl.multiple_of(j * plane_rows, plane_rows), plane_rows))
            return carry

        lax.fori_loop(group.start, group.stop, step, 0)

    started, done = [], {near: 0, far: 0}

    def consume(group, s):
        if not started:
            loads[1].wait()
            loads[2].wait()
            started.append(s)
        start, size = slices_of(features)[s]
        first = done[group] == 0

        def multiply(place, at):
            left = held[place, :, :, :, :, start : start + size].reshape(-1, size)
            for weight, total in ((gate, gate_sum), (up, up_sum)):
                value = jnp.dot(
                    left, weight[start : start + size, :], preferred_element_type=jnp.float32
                )
                total[at, :] = value if first else total[at, :] + value

        over(group, multiply)
        done[group] += 1
        if done[group] == slices:
            over(group, activate)

    expert = (here.ep * depth + here.z) // 2

    def activate(place, at):
        tail = wide(held[place, :, :, :, :, features:].reshape(-1, tail_width))
        lane = lax.broadcasted_iota(jnp.int32, tail.shape, 1)
        weight = jnp.sum(jnp.where(lane == expert, tail, 0.0), axis=1, keepdims=True)
        scale = jnp.sum(
            jnp.where((lane == experts) | (lane == experts + 1), tail, 0.0), axis=1, keepdims=True
        )
        gate_val = gate_sum[at, :] * scale
        value = gate_val / (1.0 + jnp.exp(-gate_val)) * (up_sum[at, :] * (scale * weight))
        act[at, :] = value.astype(jnp.bfloat16)

    in1, in2, in3, in4 = scratch[3:7]
    proj_buffers, expert_buffers, sems = scratch[:3], scratch[3:6], scratch[7:]
    near_sems, far_sems, near_gather_sems, far_gather_sems = sems[:4], sems[4:8], sems[8:11], sems[11:14]
    fsem, fsent = sems[14:]

    def proj_parts(y, x, core, cols, place=None):
        return in1.at[pl.ds(core, 1), y, x, :, cols]

    def expert_parts(group):
        return lambda y, x, core, cols, place=group: held.at[place, y, x, core, :, cols]

    def produce(group):
        def run(s, cols, put):
            if not waited[group]:
                if group is near:
                    loads[3].wait()
                    wait_reduce()
                    wait_bytes(held.at[far, 0, 0, 0], zsent.at[0])
                (wait_near if group is near else wait_far)()
                waited[group].append(s)

            def multiply(place, at):
                put(jnp.dot(act[at, :], down[:, cols], preferred_element_type=jnp.float32), place)

            over(group, multiply)

        return run

    waited = {near: [], far: []}
    halves = [0] * slices

    def settle(s, cols, total):
        mixed[:, cols] = (mixed if halves[s] else hidden)[:, cols] + total
        halves[s] += 1

    def finish_near(s, cols, total):
        settle(s, cols, total[0])

    def finish_far(s, cols, total):
        in1[far, here.y, here.x, :, cols] = total.astype(jnp.bfloat16)
        for j in range(1, depth):
            remote(
                in1.at[j, here.y, here.x, :, cols],
                in4.at[j - 1, :, cols],
                fsent.at[0],
                fsem.at[s],
                here.at(0, 0, j),
            ).start()

    def finish_layer(s):
        cols = pl.ds(*slices_of(features)[s])
        wait_bytes(in4.at[:, :, cols], fsem.at[s])
        settle(s, cols, sum(wide(in4[j, :, cols]) for j in range(depth - 1)))

    reduced = []

    def finish_first(s, cols, total):
        if not reduced:
            wait_core()
        reduced.append(s)
        finish_proj(s, cols, total[0])

    reduce, wait_core, wait_reduce = reduce_phases(
        flat, near, rows, features, produce_proj, finish_first, proj_parts, proj_buffers, near_sems
    )
    near_gather, wait_near = gather_phases(here, held, near, features, near_gather_sems)
    far_gather, wait_far = gather_phases(here, held, far, features, far_gather_sems)
    near_spread, wait_near_core, wait_near_spread = reduce_phases(
        here, near, rows, features, produce(near), finish_near, expert_parts(near), expert_buffers, near_sems
    )
    far_spread, wait_far_core, wait_far_spread = reduce_phases(
        here, far, rows, features, produce(far), finish_far, expert_parts(far), expert_buffers, far_sems
    )

    def use(arrive, group):
        def run(s):
            arrive(s)
            consume(group, s)

        return run

    tasks = (
        *reduce,
        near_gather[1], near_gather[2], use(near_gather[3], near),
        relay, far_gather[1], far_gather[2], use(far_gather[3], far),
        *near_spread, *far_spread, finish_layer,
    )
    for task, s in task_order(slices):
        with jax.named_scope(f"t{task}_{s}"):
            tasks[task](s)
    wait_near_core()
    wait_near_spread()
    wait_far_core()
    wait_far_spread()
    wait_bytes(in1.at[far, 0, 0], fsent.at[0])
    wait_bytes(regrouped.at[0 : count - 1], xsem.at[0])


def nt_dot(left, right):
    return lax.dot_general(left, right, (((1,), (1,)), ((), ())), preferred_element_type=jnp.float32)


PAD = 16


def run_layer(
    side, depth, lengths, queries, new_keys, new_values, resid, gain, router, named_ids,
    cache_keys, cache_values, out_proj, gate_slab, up_slab, down_slab
):
    rows, width = resid.shape
    n = len(slices_of(width))
    experts = router.shape[0]
    span = cache_keys.shape[1]
    bf, dma = jnp.bfloat16, pltpu.SemaphoreType.DMA
    plane = 2 * side * side
    count = plane * depth
    tail = pl.cdiv(experts + 2, 128) * 128
    vmem, anywhere = pl.BlockSpec(memory_space=pltpu.VMEM), pl.BlockSpec(memory_space=pl.ANY)
    return pl.pallas_call(
        lambda *refs: layer_kernel(side, depth, *refs),
        out_shape=jax.ShapeDtypeStruct((rows, width), jnp.float32),
        in_specs=[pl.BlockSpec(memory_space=pltpu.SMEM)] + [vmem] * 7 + [anywhere] * 6,
        out_specs=vmem,
        scratch_shapes=[
            pltpu.VMEM((rows, span + PAD, KVH * HD), bf),
            pltpu.VMEM((rows, span + PAD, KVH * HD), bf),
            pltpu.VMEM((H // KVH * rows, HD), jnp.float32),
            pltpu.VMEM((H // KVH * rows, HD), jnp.float32),
            pltpu.VMEM((rows, H * HD), bf),
            pltpu.VMEM(out_proj.shape, bf),
            pltpu.VMEM(gate_slab.shape[1:], bf),
            pltpu.VMEM(up_slab.shape[1:], bf),
            pltpu.VMEM(down_slab.shape[1:], bf),
            pltpu.VMEM((plane, rows, H * HD // plane), bf),
            pltpu.VMEM((rows, width), jnp.float32),
            pltpu.VMEM((depth, side, side, 2, rows, width + tail), bf),
            pltpu.VMEM((count * rows, gate_slab.shape[2]), bf),
            pltpu.VMEM((count * rows, gate_slab.shape[2]), jnp.float32),
            pltpu.VMEM((count * rows, gate_slab.shape[2]), jnp.float32),
            dma((2, KVH)),
            dma((4,)),
            dma((2,)),
            dma((n,)),
            dma((1,)),
        ]
        + reduce_shapes(side, 1, rows, width)
        + reduce_shapes(side, depth, rows, width)
        + [pltpu.VMEM((depth - 1, rows, width), bf)]
        + reduce_sems(side, n) * 2
        + [dma((3,)), dma((n, side * side - 1)), dma((n,))] * 2
        + [dma((n,)), dma((1,))],
        compiler_params=pltpu.CompilerParams(
            collective_id=0, has_side_effects=True, vmem_limit_bytes=VMEM_LIMIT
        ),
    )(
        lengths, queries, new_keys, new_values, resid, gain, router, named_ids,
        cache_keys, cache_values, out_proj, gate_slab, up_slab, down_slab,
    )


def local(
    resid,
    queries,
    new_keys,
    new_values,
    cache_keys,
    cache_values,
    cache_len,
    out_proj,
    norm_gain,
    router,
    expert_ids,
    gate_slab,
    up_slab,
    down_slab,
):
    side = math.isqrt(lax.axis_size("ep") // 2)
    depth = lax.axis_size("dp")
    return run_layer(
        side, depth, cache_len, queries, new_keys, new_values, resid, norm_gain.reshape(1, -1),
        router.T, expert_ids.T, cache_keys, cache_values, out_proj, gate_slab, up_slab, down_slab,
    )


def solution(mesh):
    in_specs = (
        P(("ep", "dp"), None),
        P(("ep", "dp"), None),
        P(("ep", "dp"), None),
        P(("ep", "dp"), None),
        P(("ep", "dp"), None, None),
        P(("ep", "dp"), None, None),
        P(("ep", "dp")),
        P("ep", None),
        P(),
        P(),
        P(("ep", "dp"), None),
        P(("ep", "dp"), None, None),
        P(("ep", "dp"), None, None),
        P(("ep", "dp"), None, None),
    )
    out_specs = P(("ep", "dp"), None)
    return jax.shard_map(local, mesh=mesh, in_specs=in_specs, out_specs=out_specs, check_vma=False)
```

```python
import math

import jax
import jax.numpy as jnp
from jax import lax
from jax.experimental import pallas as pl
from jax.experimental.pallas import tpu as pltpu
from jax.sharding import PartitionSpec as P

D = 4096
H = 64
KVH = 4
HD = 128
TOP = 8


MESH = pl.DeviceIdType.MESH
VMEM_LIMIT = 67_000_000


class Place:
    def __init__(self, side, depth):
        self.side, self.depth = side, depth
        ep = lax.axis_index("ep")
        self.ep = ep
        self.core = lax.rem(ep, 2)
        self.x = lax.rem(ep // 2, side)
        self.y = ep // (2 * side)
        self.z = lax.axis_index("dp")

    def at(self, dy=0, dx=0, dz=0, flip=False):
        y, x = self.line(dy, dx)
        z = lax.rem(self.z + dz, self.depth) if dz else self.z
        core = 1 - self.core if flip else self.core
        return ((y * self.side + x) * 2 + core, z)

    def line(self, dy, dx):
        return lax.rem(self.y + dy, self.side), lax.rem(self.x + dx, self.side)


def announce(devices):
    barrier = pltpu.get_barrier_semaphore()
    for device in devices:
        pl.semaphore_signal(barrier, inc=1, device_id=device, device_id_type=MESH)


def gathered(devices):
    pl.semaphore_wait(pltpu.get_barrier_semaphore(), len(devices))


def remote(src, dst, send, recv, device):
    return pltpu.make_async_remote_copy(
        src_ref=src, dst_ref=dst, send_sem=send, recv_sem=recv, device_id=device, device_id_type=MESH
    )


SLICE = 512
STAGES = 8
ORDER = (
    2, 5, 3, 10, 1, 4, 11, 6, 7, 13, 0, 12, 8, 14, 9, 15, 26, 29, 28, 24,
    27, 25, 30, 34, 31, 36, 37, 32, 35, 58, 61, 33, 44, 39, 38, 40, 60, 66, 56, 41,
    59, 69, 42, 46, 47, 48, 45, 43, 52, 57, 55, 62, 51, 54, 74, 53, 63, 82, 65, 68,
    64, 50, 49, 88, 77, 67, 95, 92, 70, 93, 89, 71, 90, 85, 76, 101, 91, 73, 75, 98,
    72, 84, 81, 78, 99, 103, 97, 100, 96, 79, 80, 83, 86, 87, 124, 125, 106, 120, 127, 132,
    133, 126, 128, 121, 135, 122, 123, 141, 140, 130, 136, 129, 143, 134, 149, 105, 148, 138, 131, 144,
    137, 109, 107, 151, 142, 94, 146, 139, 145, 111, 150, 102, 115, 147, 108, 110, 117, 152, 104, 116,
    114, 112, 158, 159, 156, 113, 118, 157, 153, 154, 119, 155,
)


def slices_of(width):
    return [(start, SLICE) for start in range(0, width, SLICE)]


def task_order(count):
    if count == STAGES:
        return [(code // STAGES, code % STAGES) for code in ORDER]
    return [(task, s) for task in range(20) if task != 2 for s in range(count)]


def reduce_shapes(side, depth, rows, width):
    bf = jnp.bfloat16
    return [
        pltpu.VMEM((depth, side, side, rows, width), bf),
        pltpu.VMEM((depth, side - 1, side, rows, width), bf),
        pltpu.VMEM((depth, side - 1, rows, width), bf),
    ]


def reduce_sems(side, n):
    dma = pltpu.SemaphoreType.DMA
    return [dma((3,)), dma((n,)), dma((n, side - 1, side)), dma((n, side - 1))]


def wide(value):
    return value.astype(jnp.float32)


def wait_bytes(ref, sem):
    pltpu.make_async_copy(ref, ref, sem).wait()


def reduce_phases(here, group, rows, width, produce, finish, part, buffers, sems):
    in1, in2, in3 = buffers
    sent, sem1, sem2, sem3 = sems
    side = here.side
    cuts = slices_of(width)
    every = slice(None)

    def core_copy(s):
        cols = pl.ds(*cuts[s])
        return remote(
            part(every, every, 1 - here.core, cols),
            in1.at[group, :, :, :, cols],
            sent.at[0],
            sem1.at[s],
            here.at(flip=True),
        )

    def offsets(s, a, b):
        return (a, b) if s % 2 == 0 else (b, a)

    def first_copy(s, ja, kb, sending):
        cols = pl.ds(*cuts[s])
        slot = side - ja - 1
        y, x = here.line(*offsets(s, ja, kb))
        return remote(
            in1.at[group, y, x, :, cols],
            in2.at[group, slot, kb, :, cols],
            sent.at[1],
            sem2.at[s, (side - ja if sending else ja) - 1, kb],
            here.at(*offsets(s, ja, 0)),
        )

    def second_copy(s, kb, sending):
        cols = pl.ds(*cuts[s])
        y, x = here.line(*offsets(s, 0, kb))
        return remote(
            in1.at[group, y, x, :, cols],
            in3.at[group, side - kb - 1, :, cols],
            sent.at[2],
            sem3.at[s, (side - kb if sending else kb) - 1],
            here.at(*offsets(s, 0, kb)),
        )

    def phase0(s):
        cols = pl.ds(*cuts[s])

        def put(value, place):
            value = value.astype(jnp.bfloat16).reshape(-1, side, side, 2, rows, cuts[s][1])
            for core in range(2):
                part(every, every, core, cols, place)[...] = value[:, :, :, core]

        produce(s, cols, put)
        core_copy(s).start()

    def phase1(s):
        cols = pl.ds(*cuts[s])
        core_copy(s).wait_recv()
        for a in list(range(1, side)) + [0]:
            for b in list(range(1, side)) + [0]:
                y, x = here.line(*offsets(s, a, b))
                total = wide(part(y, x, here.core, cols)[...]) + wide(in1[group, y, x, :, cols])
                in1[group, y, x, :, cols] = total.astype(jnp.bfloat16)
                if a:
                    first_copy(s, a, b, True).start()

    def phase2(s):
        cols = pl.ds(*cuts[s])
        for b in list(range(1, side)) + [0]:
            y, x = here.line(*offsets(s, 0, b))
            total = wide(in1[group, y, x, :, cols])
            for a in range(1, side):
                first_copy(s, a, b, False).wait_recv()
                total = total + wide(in2[group, a - 1, b, :, cols])
            in1[group, y, x, :, cols] = total.astype(jnp.bfloat16)
            if b:
                second_copy(s, b, True).start()

    def phase3(s):
        cols = pl.ds(*cuts[s])
        total = wide(in1[group, here.y, here.x, :, cols])
        for b in range(1, side):
            second_copy(s, b, False).wait_recv()
            total = total + wide(in3[group, b - 1, :, cols])
        finish(s, cols, total)

    def wait_core():
        wait_bytes(in1.at[group], sent.at[0])

    def wait_sent():
        wait_bytes(in1.at[group, 0 : side - 1], sent.at[1])
        wait_bytes(in1.at[group, 0, 0 : side - 1], sent.at[2])

    return (phase0, phase1, phase2, phase3), wait_core, wait_sent


def direct_phases(here, rows, width, produce, finish, part, buffers, sems):
    in1, in2 = buffers
    sent, sem1, sem2 = sems
    side = here.side
    cuts = slices_of(width)
    every = slice(None)
    lines = [(a, b) for a in range(side) for b in range(side)]

    def core_copy(s):
        cols = pl.ds(*cuts[s])
        return remote(
            part(every, every, 1 - here.core, cols),
            in1.at[:, :, :, :, cols],
            sent.at[0],
            sem1.at[s],
            here.at(flip=True),
        )

    def phase0(s):
        cols = pl.ds(*cuts[s])

        def put(value):
            value = value.astype(jnp.bfloat16).reshape(1, side, side, 2, rows, cuts[s][1])
            for core in range(2):
                part(every, every, core, cols)[...] = value[:, :, :, core]

        produce(s, cols, put)
        core_copy(s).start()

    def phase1(s):
        cols = pl.ds(*cuts[s])
        core_copy(s).wait_recv()
        for a, b in reversed(lines):
            y, x = here.line(a, b)
            total = wide(part(y, x, here.core, cols)[0]) + wide(in1[0, y, x, :, cols])
            in1[0, y, x, :, cols] = total.astype(jnp.bfloat16)
            if a or b:
                slot = (side - a) % side * side + (side - b) % side - 1
                remote(
                    in1.at[0, y, x, :, cols],
                    in2.at[slot, :, cols],
                    sent.at[1],
                    sem2.at[s, 0],
                    here.at(a, b),
                ).start()

    def phase2(s):
        cols = pl.ds(*cuts[s])
        wait_bytes(in2.at[:, :, cols], sem2.at[s, 0])
        total = wide(in1[0, here.y, here.x, :, cols])
        for slot in range(side * side - 1):
            total = total + wide(in2[slot, :, cols])
        finish(s, cols, total)

    def wait_core():
        wait_bytes(in1, sent.at[0])

    def wait_sent():
        wait_bytes(in2, sent.at[1])

    return (phase0, phase1, phase2), wait_core, wait_sent


def gather_phases(here, held, group, features, sems):
    side = here.side
    sent, lsem, csem = sems
    cuts = slices_of(features)
    cuts[-1] = (cuts[-1][0], held.shape[-1] - cuts[-1][0])

    def line_ref(s, ky, kx, core):
        y, x = here.line(ky, kx)
        return held.at[group, y, x, core, :, pl.ds(*cuts[s])]

    def arrival(s, ky, kx):
        return lsem.at[s, (ky % side) * side + kx % side - 1]

    def core_send(s, ky, kx):
        ref = line_ref(s, ky, kx, here.core)
        remote(ref, ref, sent.at[2], csem.at[s], here.at(flip=True)).start()

    def plane_wait(s, ky, kx):
        wait_bytes(line_ref(s, ky, kx, here.core), arrival(s, ky, kx))

    def turn(s, a, b):
        return (a, b) if s % 2 == 0 else (b, a)

    def own_send(s):
        ref = line_ref(s, 0, 0, here.core)
        for j in range(1, side):
            for jy, jx in (turn(s, j, 0), turn(s, 0, j)):
                remote(ref, ref, sent.at[0], arrival(s, -jy, -jx), here.at(jy, jx)).start()
        core_send(s, 0, 0)

    def forward(s):
        for k in range(1, side):
            plane_wait(s, *turn(s, k, 0))
            ref = line_ref(s, *turn(s, k, 0), here.core)
            for j in range(1, side):
                jy, jx = turn(s, 0, j)
                ky, kx = turn(s, k, 0)
                remote(ref, ref, sent.at[1], arrival(s, ky - jy, kx - jx), here.at(jy, jx)).start()
            core_send(s, *turn(s, k, 0))

    def collect(s):
        for b in range(1, side):
            for a in range(side):
                plane_wait(s, *turn(s, a, b))
                core_send(s, *turn(s, a, b))

    def arrive(s):
        wait_bytes(held.at[group, :, :, 1 - here.core, :, pl.ds(*cuts[s])], csem.at[s])

    def wait_sent():
        wait_bytes(held.at[group, 0 : side - 1, 0:2, 0], sent.at[0])
        wait_bytes(held.at[group, 0 : side - 1, 0 : side - 1, 0], sent.at[1])
        wait_bytes(held.at[group, :, :, 0], sent.at[2])

    return (own_send, forward, collect, arrive), wait_sent


def layer_kernel(
    side, depth, lengths, queries_hbm, new_keys_hbm, new_values_hbm, resid_hbm, gain_hbm, router_hbm, ids_hbm,
    keys_hbm, values_hbm, proj_hbm, gate_hbm, up_hbm, down_hbm, mixed,
    queries, new_keys, new_values, resid, gain, router, named_ids, isem, keys, values, query_rows, blend_rows, attended,
    proj, gate, up, down, regrouped, hidden, held, act, gate_sum, up_sum,
    ksem, wsem, xsem, zsem, zsent, *scratch
):
    here, flat = Place(side, depth), Place(side, 1)
    rows, features = resid.shape
    experts = router.shape[0]
    count = 2 * side * side
    width = attended.shape[1] // count
    span = keys_hbm.shape[1]
    group_size = H // KVH
    pieces = count // KVH
    own_group = here.ep // pieces

    def peer(j):
        return lax.rem(here.ep + j, count)

    peers = [(peer(j), here.z) for j in range(1, count)] + [here.at(0, 0, j) for j in range(1, depth)]
    announce(peers)
    inputs = [
        pltpu.make_async_copy(src, dst, isem.at[i])
        for i, (src, dst) in enumerate(
            (
                (queries_hbm, queries), (new_keys_hbm, new_keys), (new_values_hbm, new_values),
                (resid_hbm, resid), (gain_hbm, gain), (router_hbm, router), (ids_hbm, named_ids),
            )
        )
    ]
    for copy in inputs[:3]:
        copy.start()

    def turn_group(i):
        return lax.rem(own_group + 1 + i, KVH)

    def lanes(g):
        return pl.ds(pl.multiple_of(g * HD, HD), HD)

    def cache_copies(i):
        return [
            pltpu.make_async_copy(
                src.at[:, :, lanes(turn_group(i))], dst.at[:, 0:span, lanes(turn_group(i))], ksem.at[n, i]
            )
            for n, (src, dst) in enumerate(((keys_hbm, keys), (values_hbm, values)))
        ]

    for i in range(KVH):
        for copy in cache_copies(i):
            copy.start()
    loads = [
        pltpu.make_async_copy(src, dst, wsem.at[i])
        for i, (src, dst) in enumerate(
            ((proj_hbm, proj), (gate_hbm.at[0], gate), (up_hbm.at[0], up), (down_hbm.at[0], down))
        )
    ]
    for copy in inputs[3:]:
        copy.start()
    loads[0].start()

    first = lax.broadcasted_iota(jnp.int32, (PAD, KVH * HD), 0) == 0
    for copy in inputs[:3]:
        copy.wait()
    for new, cache in ((new_keys, keys), (new_values, values)):
        wide_new = new[...].astype(jnp.float32)
        for token in range(rows):
            own = jnp.where(first, wide_new[token : token + 1, :], 0.0)
            cache[token, span:, :] = own.astype(jnp.bfloat16)

    def piece(index):
        return attended.at[:, pl.ds(pl.multiple_of(index * width, 128), width)]

    def exchange(to, source):
        return remote(piece(to), regrouped.at[source], xsem.at[0], xsem.at[1], (to, here.z))

    def attend(i):
        g = turn_group(i)
        for copy in cache_copies(i):
            copy.wait()
        for h in range(group_size):
            query_rows[h * rows : (h + 1) * rows, :] = wide(queries[:, lanes(g * group_size + h)])
        scores = []
        place = lax.broadcasted_iota(jnp.int32, (group_size, span + PAD), 1)
        for token in range(rows):
            query = query_rows[pl.ds(token, group_size, stride=rows), :]
            score = nt_dot(query.astype(jnp.bfloat16), keys[token, :, lanes(g)])
            kept = (place < lengths[token]) | (place == span)
            scores.append(jnp.where(kept, score * (1.0 / math.sqrt(HD)), -1e30))
        score = jnp.concatenate(scores, axis=0)
        grown = jnp.exp(score - jnp.max(score, axis=1, keepdims=True))
        weights = (grown / jnp.sum(grown, axis=1, keepdims=True)).astype(jnp.bfloat16)
        for token in range(rows):
            blend_rows[pl.ds(token, group_size, stride=rows), :] = jnp.dot(
                weights[token * group_size : (token + 1) * group_size, :],
                values[token, :, lanes(g)],
                preferred_element_type=jnp.float32,
            )
        for h in range(group_size):
            attended[:, lanes(g * group_size + h)] = blend_rows[h * rows : (h + 1) * rows, :].astype(
                jnp.bfloat16
            )

    for i in range(KVH):
        if i == KVH - 1:
            gathered(peers)
            for load in loads[1:]:
                load.start()
            for sent in range(i):
                for k in range(pieces):
                    exchange(turn_group(sent) * pieces + k, here.ep).start()
        attend(i)
    for k in range(1, pieces):
        exchange(own_group * pieces + lax.rem(here.ep + k, pieces), here.ep).start()
    regrouped[here.ep] = attended[:, pl.ds(pl.multiple_of(here.ep * width, 128), width)]

    for copy in inputs[3:]:
        copy.wait()
    eye = jnp.where(
        lax.broadcasted_iota(jnp.int32, (rows, rows), 0) == lax.broadcasted_iota(jnp.int32, (rows, rows), 1), 1.0, 0.0
    ).astype(jnp.bfloat16)
    label = lax.broadcasted_iota(jnp.int32, (experts, rows), 0)
    hits = jnp.zeros((experts, rows), jnp.float32)
    for k in range(TOP):
        hits = hits + jnp.where(label == named_ids[k : k + 1, :], 1.0, 0.0)
    named = nt_dot(eye, hits.astype(jnp.bfloat16)) > 0.5

    loads[0].wait()
    with jax.named_scope("exchange_wait"):
        wait_bytes(regrouped.at[0 : count - 1], xsem.at[1])

    def produce_proj(s, cols, put):
        left = regrouped[...].reshape(count * rows, width)
        put(jnp.dot(left, proj[:, cols], preferred_element_type=jnp.float32))

    squares, logits = [], []
    slices = len(slices_of(features))
    tail_width = held.shape[-1] - features

    def finish_proj(s, cols, total):
        value = resid[:, cols].astype(jnp.float32) + total
        hidden[:, cols] = value
        scaled = (value * gain[:, cols]).astype(jnp.bfloat16)
        held[0, here.y, here.x, here.core, :, cols] = scaled
        if s < slices - 1:
            launch(s)
        squares.append(jnp.sum(value * value, axis=1, keepdims=True))
        logits.append(nt_dot(scaled, router[:, cols]))
        if s == slices - 1:
            scale = lax.rsqrt(jnp.maximum(sum(squares) / features, 0.25))
            scores = sum(logits) * scale
            peak = jnp.max(jnp.where(named, scores, -jnp.inf), axis=1, keepdims=True)
            grown = jnp.where(named, jnp.exp(jnp.where(named, scores - peak, 0.0)), 0.0)
            probs = grown / jnp.sum(grown, axis=1, keepdims=True)
            high = scale.astype(jnp.bfloat16).astype(jnp.float32)
            lane = lax.broadcasted_iota(jnp.int32, (rows, tail_width), 1)
            tail = jnp.where(lane == experts, high, jnp.where(lane == experts + 1, scale - high, 0.0))
            held[0, here.y, here.x, here.core, :, features:] = tail.astype(jnp.bfloat16)
            held[0, here.y, here.x, here.core, :, features : features + experts] = probs.astype(jnp.bfloat16)
            launch(s)

    near, far = slice(0, 1), slice(1, depth)
    plane_rows = count * rows

    def launch(s):
        start, size = slices_of(features)[s]
        cols = pl.ds(start, size if s < slices - 1 else held.shape[-1] - start)
        for j in range(1, depth):
            remote(
                held.at[0, here.y, here.x, here.core, :, cols],
                held.at[depth - j, here.y, here.x, here.core, :, cols],
                zsent.at[0],
                zsem.at[s],
                here.at(0, 0, j),
            ).start()
        near_gather[0](s)

    def relay(s):
        start, size = slices_of(features)[s]
        cols = pl.ds(start, size if s < slices - 1 else held.shape[-1] - start)
        wait_bytes(held.at[far, here.y, here.x, here.core, :, cols], zsem.at[s])
        far_gather[0](s)

    def over(group, body):
        height = plane_rows * (group.stop - group.start)
        if height <= 512:
            body(group, pl.ds(group.start * plane_rows, height))
            return

        def step(j, carry):
            body(pl.ds(j, 1), pl.ds(pl.multiple_of(j * plane_rows, plane_rows), plane_rows))
            return carry

        lax.fori_loop(group.start, group.stop, step, 0)

    started, done = [], {near: 0, far: 0}

    def consume(group, s):
        if not started:
            loads[1].wait()
            loads[2].wait()
            started.append(s)
        start, size = slices_of(features)[s]
        first = done[group] == 0

        def multiply(place, at):
            left = held[place, :, :, :, :, start : start + size].reshape(-1, size)
            for weight, total in ((gate, gate_sum), (up, up_sum)):
                value = jnp.dot(
                    left, weight[start : start + size, :], preferred_element_type=jnp.float32
                )
                total[at, :] = value if first else total[at, :] + value

        over(group, multiply)
        done[group] += 1
        if done[group] == slices:
            over(group, activate)

    expert = (here.ep * depth + here.z) // 2

    def activate(place, at):
        tail = wide(held[place, :, :, :, :, features:].reshape(-1, tail_width))
        lane = lax.broadcasted_iota(jnp.int32, tail.shape, 1)
        weight = jnp.sum(jnp.where(lane == expert, tail, 0.0), axis=1, keepdims=True)
        scale = jnp.sum(
            jnp.where((lane == experts) | (lane == experts + 1), tail, 0.0), axis=1, keepdims=True
        )
        gate_val = gate_sum[at, :] * scale
        value = gate_val / (1.0 + jnp.exp(-gate_val)) * (up_sum[at, :] * (scale * weight))
        act[at, :] = value.astype(jnp.bfloat16)

    in1, in2, in3, in4 = scratch[2:6]
    proj_buffers, expert_buffers, sems = scratch[:2], scratch[2:5], scratch[6:]
    near_sems, far_sems, near_gather_sems, far_gather_sems = sems[:4], sems[4:8], sems[8:11], sems[11:14]
    fsem, fsent = sems[14:]

    def proj_parts(y, x, core, cols):
        return in1.at[pl.ds(core, 1), y, x, :, cols]

    def expert_parts(group):
        return lambda y, x, core, cols, place=group: held.at[place, y, x, core, :, cols]

    def produce(group):
        def run(s, cols, put):
            if not waited[group]:
                if group is near:
                    loads[3].wait()
                    wait_reduce()
                    wait_bytes(held.at[far, 0, 0, 0], zsent.at[0])
                (wait_near if group is near else wait_far)()
                waited[group].append(s)

            def multiply(place, at):
                put(jnp.dot(act[at, :], down[:, cols], preferred_element_type=jnp.float32), place)

            over(group, multiply)

        return run

    waited = {near: [], far: []}
    halves = [0] * slices

    def settle(s, cols, total):
        mixed[:, cols] = (mixed if halves[s] else hidden)[:, cols] + total
        halves[s] += 1

    def finish_near(s, cols, total):
        settle(s, cols, total[0])

    def finish_far(s, cols, total):
        in1[far, here.y, here.x, :, cols] = total.astype(jnp.bfloat16)
        for j in range(1, depth):
            remote(
                in1.at[j, here.y, here.x, :, cols],
                in4.at[j - 1, :, cols],
                fsent.at[0],
                fsem.at[s],
                here.at(0, 0, j),
            ).start()

    def finish_layer(s):
        cols = pl.ds(*slices_of(features)[s])
        wait_bytes(in4.at[:, :, cols], fsem.at[s])
        settle(s, cols, sum(wide(in4[j, :, cols]) for j in range(depth - 1)))

    reduced = []

    def finish_first(s, cols, total):
        if not reduced:
            wait_core()
        reduced.append(s)
        finish_proj(s, cols, total)

    reduce, wait_core, wait_reduce = direct_phases(
        flat, rows, features, produce_proj, finish_first, proj_parts, proj_buffers,
        (near_sems[0], near_sems[1], near_sems[3]),
    )
    near_gather, wait_near = gather_phases(here, held, near, features, near_gather_sems)
    far_gather, wait_far = gather_phases(here, held, far, features, far_gather_sems)
    near_spread, wait_near_core, wait_near_spread = reduce_phases(
        here, near, rows, features, produce(near), finish_near, expert_parts(near), expert_buffers, near_sems
    )
    far_spread, wait_far_core, wait_far_spread = reduce_phases(
        here, far, rows, features, produce(far), finish_far, expert_parts(far), expert_buffers, far_sems
    )

    def use(arrive, group):
        def run(s):
            arrive(s)
            consume(group, s)

        return run

    tasks = (
        reduce[0], reduce[1], None, reduce[2],
        near_gather[1], near_gather[2], use(near_gather[3], near),
        relay, far_gather[1], far_gather[2], use(far_gather[3], far),
        *near_spread, *far_spread, finish_layer,
    )
    for task, s in task_order(slices):
        with jax.named_scope(f"t{task}_{s}"):
            tasks[task](s)
    wait_near_core()
    wait_near_spread()
    wait_far_core()
    wait_far_spread()
    wait_bytes(in1.at[far, 0, 0], fsent.at[0])
    wait_bytes(regrouped.at[0 : count - 1], xsem.at[0])


def nt_dot(left, right):
    return lax.dot_general(left, right, (((1,), (1,)), ((), ())), preferred_element_type=jnp.float32)


PAD = 16


def run_layer(
    side, depth, lengths, queries, new_keys, new_values, resid, gain, router, named_ids,
    cache_keys, cache_values, out_proj, gate_slab, up_slab, down_slab
):
    rows, width = resid.shape
    n = len(slices_of(width))
    experts = router.shape[0]
    span = cache_keys.shape[1]
    bf, dma = jnp.bfloat16, pltpu.SemaphoreType.DMA
    plane = 2 * side * side
    count = plane * depth
    tail = pl.cdiv(experts + 2, 128) * 128
    vmem, anywhere = pl.BlockSpec(memory_space=pltpu.VMEM), pl.BlockSpec(memory_space=pl.ANY)
    return pl.pallas_call(
        lambda *refs: layer_kernel(side, depth, *refs),
        out_shape=jax.ShapeDtypeStruct((rows, width), jnp.float32),
        in_specs=[pl.BlockSpec(memory_space=pltpu.SMEM)] + [anywhere] * 13,
        out_specs=vmem,
        scratch_shapes=[
            pltpu.VMEM(array.shape, array.dtype)
            for array in (queries, new_keys, new_values, resid, gain, router, named_ids)
        ]
        + [
            dma((7,)),
            pltpu.VMEM((rows, span + PAD, KVH * HD), bf),
            pltpu.VMEM((rows, span + PAD, KVH * HD), bf),
            pltpu.VMEM((H // KVH * rows, HD), jnp.float32),
            pltpu.VMEM((H // KVH * rows, HD), jnp.float32),
            pltpu.VMEM((rows, H * HD), bf),
            pltpu.VMEM(out_proj.shape, bf),
            pltpu.VMEM(gate_slab.shape[1:], bf),
            pltpu.VMEM(up_slab.shape[1:], bf),
            pltpu.VMEM(down_slab.shape[1:], bf),
            pltpu.VMEM((plane, rows, H * HD // plane), bf),
            pltpu.VMEM((rows, width), jnp.float32),
            pltpu.VMEM((depth, side, side, 2, rows, width + tail), bf),
            pltpu.VMEM((count * rows, gate_slab.shape[2]), bf),
            pltpu.VMEM((count * rows, gate_slab.shape[2]), jnp.float32),
            pltpu.VMEM((count * rows, gate_slab.shape[2]), jnp.float32),
            dma((2, KVH)),
            dma((4,)),
            dma((2,)),
            dma((n,)),
            dma((1,)),
        ]
        + [
            pltpu.VMEM((1, side, side, rows, width), bf),
            pltpu.VMEM((side * side - 1, rows, width), bf),
        ]
        + reduce_shapes(side, depth, rows, width)
        + [pltpu.VMEM((depth - 1, rows, width), bf)]
        + reduce_sems(side, n) * 2
        + [dma((3,)), dma((n, side * side - 1)), dma((n,))] * 2
        + [dma((n,)), dma((1,))],
        compiler_params=pltpu.CompilerParams(
            collective_id=0, has_side_effects=True, vmem_limit_bytes=VMEM_LIMIT
        ),
    )(
        lengths, queries, new_keys, new_values, resid, gain, router, named_ids,
        cache_keys, cache_values, out_proj, gate_slab, up_slab, down_slab,
    )


def local(
    resid,
    queries,
    new_keys,
    new_values,
    cache_keys,
    cache_values,
    cache_len,
    out_proj,
    norm_gain,
    router,
    expert_ids,
    gate_slab,
    up_slab,
    down_slab,
):
    side = math.isqrt(lax.axis_size("ep") // 2)
    depth = lax.axis_size("dp")
    return run_layer(
        side, depth, cache_len, queries, new_keys, new_values, resid, norm_gain.reshape(1, -1),
        router.T, expert_ids.T, cache_keys, cache_values, out_proj, gate_slab, up_slab, down_slab,
    )


def solution(mesh):
    in_specs = (
        P(("ep", "dp"), None),
        P(("ep", "dp"), None),
        P(("ep", "dp"), None),
        P(("ep", "dp"), None),
        P(("ep", "dp"), None, None),
        P(("ep", "dp"), None, None),
        P(("ep", "dp")),
        P("ep", None),
        P(),
        P(),
        P(("ep", "dp"), None),
        P(("ep", "dp"), None, None),
        P(("ep", "dp"), None, None),
        P(("ep", "dp"), None, None),
    )
    out_specs = P(("ep", "dp"), None)
    return jax.shard_map(local, mesh=mesh, in_specs=in_specs, out_specs=out_specs, check_vma=False)
```
